32 devices in a mesh: scene: 2 (over x), view: 16 (over z, y, core).
Axes of the slice: x: 2, y: 2, z: 4, core: 2. Of those that a mesh axis runs over, the one named last changes fastest.
Arguments:
- latents: bfloat16 [256, 64, 512], P(('scene', 'view')), parts along dimension 0, may hold values from -48 to 48
- norm_gain: float32 [512], replicated, may hold values from 0.1 to 1.9
- norm_shift: float32 [512], replicated, may hold values from -3 to 3
- w_first: bfloat16 [512, 3, 3, 512], replicated, may hold values from -0.09375 to 0.09375
- bias_first: float32 [512], replicated, may hold values from -3 to 3
- w_second: bfloat16 [512, 3, 3, 512], replicated, may hold values from -0.09375 to 0.09375
- bias_second: float32 [512], replicated, may hold values from -3 to 3
Outputs:
- decoded: bfloat16 [512, 128, 512], P(('scene', 'view')), parts along dimension 0
The draws below stay inside these ranges and needn't reach their ends.
There are 2 independent parts, one for each index of `scene`. The reference program is written for one: setup_inputs(seed, part) draws one part's arguments, and reference() takes and returns one part's arrays. A program takes and returns all parts, laid end to end along the dimension named above; an argument that names none is the same for every part. Nothing has to cross between parts.
All inputs are finite; a program needn't handle non-finite values.
Results may differ from the reference program's by a relative error of at most 0.0051.
Values may be sent and summed in bfloat16 or wider, within the bound.
A program may use at most 128 MiB of HBM per device.

```python
import jax
import jax.numpy as jnp
from jax import lax

C = 512
GROUPS = 32
ROWS_DEV = 8
H_LAT = 32
W_LAT = 64
SLABS = 4
VIEWS = 4


def draw_latents(key, part):
    total_rows = VIEWS * H_LAT
    block_count = total_rows // ROWS_DEV
    key_noise = jax.random.fold_in(key, 11)
    key_scale = jax.random.fold_in(key, 23)
    key_level = jax.random.fold_in(key, 37)
    key_sign = jax.random.fold_in(key, 41)
    key_jitter = jax.random.fold_in(key, 53)
    key_block_sign = jax.random.fold_in(key, 61)
    key_block_level = jax.random.fold_in(key, 67)
    key_block_noise = jax.random.fold_in(key, 71)
    noise = jnp.clip(jax.random.normal(key_noise, (total_rows, W_LAT, C), jnp.float32), -4.0, 4.0)
    place = jnp.arange(total_rows, dtype=jnp.float32) / (total_rows - 1)
    level = jax.random.uniform(key_level, (GROUPS,), jnp.float32, 0.5, 1.5)
    sign = jnp.where(jax.random.uniform(key_sign, (GROUPS,), jnp.float32) < 0.5, -1.0, 1.0)
    block_sign = jnp.where(jax.random.uniform(key_block_sign, (block_count, GROUPS), jnp.float32) < 0.5, -1.0, 1.0)
    chan_jitter = jax.random.uniform(key_jitter, (C,), jnp.float32, 0.7, 1.3)
    row_scale = 3.0 ** (place - 0.5)
    chan_scale = 2.0 ** (2.0 * jax.random.uniform(key_scale, (C,), jnp.float32) - 1.0)
    rise = 1.0 + 2.0 * place
    block_level = jax.random.uniform(key_block_level, (block_count, GROUPS), jnp.float32, 0.3, 1.7)
    block_noise = jax.random.uniform(key_block_noise, (block_count,), jnp.float32, 0.5, 1.5)
    common = 0.5
    block_group = common * (level * sign)[None, :] + block_sign * block_level
    block_shift = jnp.broadcast_to(block_group[:, :, None], (block_count, GROUPS, C // GROUPS)).reshape(block_count, C) * chan_jitter
    row_shift = jnp.repeat(block_shift, ROWS_DEV, axis=0)
    row_noise = jnp.repeat(block_noise, ROWS_DEV, axis=0)
    values = noise * (row_scale * row_noise)[:, None, None] * chan_scale + rise[:, None, None] * row_shift[:, None, :]
    values = jnp.clip(0.35 * values, -48.0, 48.0)
    return values.astype(jnp.bfloat16)


def normal_values(key, shape, spread, most, kind=jnp.bfloat16):
    entries = spread * jax.random.normal(key, shape, jnp.float32)
    return jnp.clip(entries, min=-most, max=most).astype(kind)


def setup_inputs(seed: int = 0, part: int = 0) -> dict:
    key_of = jax.random.split(jax.random.key(seed), 8)
    part_keys = jax.random.split(jax.random.fold_in(key_of[7], part), 8)
    latents = draw_latents(jax.random.fold_in(jax.random.fold_in(key_of[7], part), 71), part)
    norm_gain = jnp.clip(1.0 + 0.18 * jax.random.normal(key_of[1], (C,), jnp.float32), 0.1, 1.9)
    norm_shift = normal_values(key_of[2], (C,), 0.5, 3.0, jnp.float32)
    w_first = normal_values(key_of[3], (C, 3, 3, C), (9 * C) ** -0.5, 0.09375)
    bias_first = normal_values(key_of[4], (C,), 0.5, 3.0, jnp.float32)
    w_second = normal_values(key_of[5], (C, 3, 3, C), (9 * C) ** -0.5, 0.09375)
    bias_second = normal_values(key_of[6], (C,), 0.5, 3.0, jnp.float32)
    return dict(latents=latents, norm_gain=norm_gain, norm_shift=norm_shift, w_first=w_first, bias_first=bias_first, w_second=w_second, bias_second=bias_second)


epsilon = 1e-06

def convolve(inputs, filters):
    return lax.conv_general_dilated(inputs.astype(jnp.float32), filters.astype(jnp.float32), (1, 1), ((1, 1), (1, 1)), dimension_numbers=('NHWC', 'OHWI', 'NHWC'), precision=lax.Precision.HIGHEST)

def reference(latents, norm_gain, norm_shift, w_first, bias_first, w_second, bias_second):
    per_group = C // GROUPS
    values = latents.astype(jnp.float32).reshape(SLABS, VIEWS, ROWS_DEV, W_LAT, C)
    values = jnp.transpose(values, (1, 0, 2, 3, 4)).reshape(VIEWS, H_LAT, W_LAT, C)
    grouped = values.reshape(VIEWS, H_LAT, W_LAT, GROUPS, per_group)
    group_mean = lax.optimization_barrier(jnp.mean(grouped, axis=(0, 1, 2, 4), keepdims=True))
    group_var = lax.optimization_barrier(jnp.mean(jnp.square(grouped - group_mean), axis=(0, 1, 2, 4), keepdims=True))
    normed = ((grouped - group_mean) * lax.rsqrt(group_var + epsilon)).reshape(VIEWS, H_LAT, W_LAT, C)
    active = jax.nn.silu(normed * norm_gain + norm_shift).astype(jnp.bfloat16)
    mixed = (values + convolve(active, w_first) + bias_first).astype(jnp.bfloat16)
    doubled = jnp.repeat(jnp.repeat(mixed, 2, axis=1), 2, axis=2)
    decoded = (convolve(doubled, w_second) + bias_second).astype(jnp.bfloat16)
    decoded = decoded.reshape(VIEWS, SLABS, 2 * ROWS_DEV, 2 * W_LAT, C)
    decoded = jnp.transpose(decoded, (1, 0, 2, 3, 4))
    return decoded.reshape(VIEWS * 2 * H_LAT, 2 * W_LAT, C)
```

```python
import functools

import jax
import jax.numpy as jnp
from jax import lax
from jax.experimental import pallas as pl
from jax.experimental.pallas import tpu as pltpu
from jax.sharding import PartitionSpec as P

GROUPS = 32
H_LAT = 32
EPSILON = 1e-06
LANES = 128
TILE = 256
F32 = jnp.float32
BF16 = jnp.bfloat16


def dot_nt(x, w):
    return lax.dot_general(x, w, (((1,), (1,)), ((), ())), preferred_element_type=F32)


def dot_nn(x, w):
    return lax.dot_general(x, w, (((1,), (0,)), ((), ())), preferred_element_type=F32)


def kernel(
    n_view, rows, cols, chans,
    lat_hbm, gain_hbm, shift_hbm, w1_hbm, b1_hbm, w2_hbm, b2_hbm,
    out_ref,
    lat, small, w1, gt, w2, fold, act, vbuf, mbuf, mx, lhs_m, lhs_u, part, wide, stat, stat_in,
    lat_sem, small_sem, w1_sem, w2_sem, halo_send, halo_recv, stat_send, stat_recv,
):
    me = lax.axis_index("view")
    slabs = H_LAT // rows
    views = n_view // slabs
    slab = me // views
    own = rows * cols
    has_up = slab > 0
    has_down = slab < slabs - 1

    barrier = pltpu.get_barrier_semaphore()

    def greet(k, carry):
        pl.semaphore_signal(barrier, inc=1, device_id={"view": lax.rem(me + k, n_view)})
        return carry

    def lat_copy(i):
        return pltpu.make_async_copy(lat_hbm.at[i], lat.at[2 + i], lat_sem.at[i])

    def small_copy(i):
        ref = (gain_hbm, shift_hbm, b1_hbm, b2_hbm)[i]
        return pltpu.make_async_copy(ref, small.at[i], small_sem.at[i])

    def w1_copy(t):
        return pltpu.make_async_copy(w1_hbm.at[t], w1.at[t], w1_sem.at[t])

    def w2_copy(t):
        return pltpu.make_async_copy(w2_hbm.at[t], w2.at[t], w2_sem.at[t])

    for i in range(rows):
        lat_copy(i).start()
    lax.fori_loop(1, n_view, greet, 0, unroll=n_view <= 16)
    for t in range(9):
        w1_copy(t).start()
    for i in range(4):
        small_copy(i).start()
    for t in range(9):
        w2_copy(t).start()

    sums = jnp.zeros((8, chans), F32)
    squares = jnp.zeros((8, chans), F32)
    for i in range(rows):
        lat_copy(i).wait()
        x = lat[2 + i].astype(F32).reshape(cols // 8, 8, chans)
        sums = sums + jnp.sum(x, axis=0)
        squares = squares + jnp.sum(x * x, axis=0)
    sums = jnp.sum(sums, axis=0, keepdims=True)
    squares = jnp.sum(squares, axis=0, keepdims=True)
    blocks = chans // LANES
    stat[...] = jnp.concatenate(
        [v[:, k * LANES : (k + 1) * LANES] for v in (sums, squares) for k in range(blocks)], axis=0
    )

    pl.semaphore_wait(barrier, n_view - 1)

    def send_stat(k, carry):
        to = k + (k >= me).astype(jnp.int32)
        slot = lax.rem(to - me + n_view, n_view) - 1
        pltpu.make_async_remote_copy(
            src_ref=stat, dst_ref=stat_in.at[slot], send_sem=stat_send, recv_sem=stat_recv,
            device_id={"view": to},
        ).start()
        return carry

    lax.fori_loop(0, n_view - 1, send_stat, 0, unroll=n_view <= 16)

    up_copy = pltpu.make_async_remote_copy(
        src_ref=lat.at[pl.ds(2, 2)], dst_ref=lat.at[pl.ds(rows + 2, 2)],
        send_sem=halo_send.at[0], recv_sem=halo_recv.at[0],
        device_id={"view": jnp.maximum(me - views, 0)},
    )
    down_copy = pltpu.make_async_remote_copy(
        src_ref=lat.at[pl.ds(rows, 2)], dst_ref=lat.at[pl.ds(0, 2)],
        send_sem=halo_send.at[1], recv_sem=halo_recv.at[1],
        device_id={"view": jnp.minimum(me + views, n_view - 1)},
    )

    @pl.when(has_up)
    def _():
        up_copy.start()

    @pl.when(has_down)
    def _():
        down_copy.start()

    tiles = chans // TILE
    eye = (
        lax.broadcasted_iota(jnp.int32, (TILE, TILE), 0) == lax.broadcasted_iota(jnp.int32, (TILE, TILE), 1)
    ).astype(F32).astype(BF16)
    for t in range(9):
        w1_copy(t).wait()

    def prepare(j, carry):
        k_at = pl.ds(pl.multiple_of(j // tiles * TILE, TILE), TILE)
        n_at = pl.ds(pl.multiple_of(lax.rem(j, tiles) * TILE, TILE), TILE)
        for s in range(3):
            g = [w1[3 * r + s, n_at, k_at] for r in range(3)]
            gt[0, s, k_at, n_at] = dot_nt(eye, g[0]).astype(BF16)
            gt[3, s, k_at, n_at] = dot_nt(eye, g[2]).astype(BF16)
            h = [v.astype(F32) for v in g]
            even = (h[0] + h[2]) * 0.5
            odd = h[1] * 0.5
            gt[1, s, k_at, n_at] = (even + odd).astype(BF16).T
            gt[2, s, k_at, n_at] = (even - odd).astype(BF16).T
        return carry

    lax.fori_loop(0, tiles * tiles, prepare, 0)

    for t in range(9):
        w2_copy(t).wait()
    piece = 32

    def fold_piece(k, carry):
        at = pl.ds(pl.multiple_of(k * piece, piece), piece)
        w = [w2[t, at].astype(F32) for t in range(9)]
        by_col = [w[s] + w[3 + s] + w[6 + s] for s in range(3)]
        fold[0, at] = (by_col[0] + by_col[1] + by_col[2]).astype(BF16)
        fold[1, at] = by_col[0].astype(BF16)
        fold[2, at] = by_col[2].astype(BF16)
        fold[3, at] = (w[0] + w[1] + w[2]).astype(BF16)
        fold[4, at] = (w[6] + w[7] + w[8]).astype(BF16)
        return carry

    lax.fori_loop(0, chans // piece, fold_piece, 0)
    for i in range(4):
        small_copy(i).wait()

    same = (
        lax.broadcasted_iota(jnp.int32, (LANES, LANES), 0) // (chans // GROUPS)
        == lax.broadcasted_iota(jnp.int32, (LANES, LANES), 1) // (chans // GROUPS)
    ).astype(F32).astype(BF16)

    pltpu.make_async_copy(stat_in, stat_in, stat_recv).wait()

    total = stat[...] + jnp.sum(stat_in[...], axis=0)
    high = total.astype(BF16).astype(F32)
    rest = total - high
    middle = rest.astype(BF16).astype(F32)
    low = rest - middle
    parts = jnp.concatenate([high, middle, low, jnp.zeros_like(low)], axis=0).astype(BF16)
    sized = dot_nn(parts, same)
    n_stat = 2 * blocks
    total = sized[:n_stat] + sized[n_stat : 2 * n_stat] + sized[2 * n_stat : 3 * n_stat]
    entries = float(own * (chans // GROUPS) * n_view)
    mean = total[:blocks] / entries
    var = total[blocks:] / entries - mean * mean
    inv = lax.rsqrt(var + EPSILON)

    def one_row(v):
        return jnp.concatenate([v[k : k + 1] for k in range(blocks)], axis=1)

    scale = one_row(inv) * small[0]
    offset = small[1] - one_row(mean) * scale
    half_scale = scale * 0.5
    half_offset = offset * 0.5

    col = lax.broadcasted_iota(jnp.int32, (cols, chans), 0)

    def left_of(x):
        return jnp.where(col == 0, 0.0, pltpu.roll(x, 1, 0))

    def right_of(x):
        return jnp.where(col == cols - 1, 0.0, pltpu.roll(x, cols - 1, 0))

    def activate(i):
        h = lat[i].astype(F32) * half_scale + half_offset
        a = h + h * jnp.tanh(h)
        if i < 2:
            a = jnp.where(has_up, a, 0.0)
        if i >= rows + 2:
            a = jnp.where(has_down, a, 0.0)
        act[0, i] = left_of(a).astype(BF16)
        act[1, i] = a.astype(BF16)
        act[2, i] = right_of(a).astype(BF16)

    inner = list(range(1, rows // 2))
    outer = [0, rows // 2]
    place = {p: k for k, p in enumerate(inner + outer)}

    def combine(k, p):
        a, b = ((0, 2), (1, 2), (2, 1), (1, 3))[k]
        at = pl.ds(place[p] * cols, cols)
        for s in range(3):
            x, y = act[s, 2 * p + a], act[s, 2 * p + b]
            vbuf[k, s, at] = x + y if k == 1 else x - y

    def products(k, pairs):
        at = pl.ds(place[pairs[0]] * cols, len(pairs) * cols)
        terms = [dot_nn(vbuf[k, s, at], gt[k, s]) for s in range(3)]
        mbuf[k, at] = terms[0] + terms[1] + terms[2]

    for i in range(2, rows + 2):
        activate(i)
    for k in range(4):
        for p in inner:
            combine(k, p)
        products(k, inner)

    @pl.when(has_up)
    def _():
        down_copy.wait_recv()

    @pl.when(has_down)
    def _():
        up_copy.wait_recv()

    bias1 = small[2]

    def mix(i):
        p, odd = i // 2, i % 2
        at = pl.ds(place[p] * cols, cols)
        conv = mbuf[1, at] - mbuf[2, at] - mbuf[3, at] if odd else mbuf[0, at] + mbuf[1, at] + mbuf[2, at]
        m = lat[i + 1].astype(F32) + conv + bias1
        m = m.astype(BF16).astype(F32)
        if i == 0:
            m = jnp.where(has_up, m, 0.0)
        if i == rows + 1:
            m = jnp.where(has_down, m, 0.0)
        left, right = left_of(m), right_of(m)
        mx[0, i] = left.astype(BF16)
        mx[1, i] = m.astype(BF16)
        mx[2, i] = right.astype(BF16)
        if 1 <= i <= rows:
            at = pl.ds((i - 1) * cols, cols)
            lhs_m[0, at] = m.astype(BF16)
            lhs_m[1, at] = (left - m).astype(BF16)
            lhs_m[2, at] = (right - m).astype(BF16)

    def rise_of(j):
        at = pl.ds(j * cols, cols)
        left, m, right = [mx[s, j + 1].astype(F32) - mx[s, j].astype(F32) for s in range(3)]
        lhs_u[0, at] = m.astype(BF16)
        lhs_u[1, at] = (left - m).astype(BF16)
        lhs_u[2, at] = (right - m).astype(BF16)

    for i in (0, 1, rows + 2, rows + 3):
        activate(i)
    for k in range(4):
        for p in outer:
            combine(k, p)
        products(k, outer)
    for i in range(2, rows):
        mix(i)
    for j in range(2, rows - 1):
        rise_of(j)

    width = TILE
    bias2 = small[3]

    def level(n, pieces):
        lanes = pl.ds(n * width, width)
        lhs = [jnp.concatenate([lhs_m[s, pl.ds(a, b)] for a, b in pieces], axis=0) for s in range(3)]
        base = dot_nt(lhs[0], fold[0, lanes]) + bias2[:, n * width : (n + 1) * width]
        for q in range(2):
            both = base + dot_nt(lhs[1 + q], fold[1 + q, lanes])
            done = 0
            for a, b in pieces:
                part[n, q, pl.ds(a, b)] = both[done : done + b]
                done += b

    level(0, [(cols, own - 2 * cols)])
    for i in (0, 1, rows, rows + 1):
        mix(i)
    for j in (0, 1, rows - 1, rows):
        rise_of(j)
    level(0, [(0, cols), (own - cols, cols)])
    for n in range(chans // width):
        lanes = pl.ds(n * width, width)
        if n:
            level(n, [(0, own)])
        for p in range(2):
            at = pl.ds(p * cols, own)
            rise = dot_nt(lhs_u[0, at], fold[3 + p, lanes])
            for q in range(2):
                term = rise + dot_nt(lhs_u[1 + q, at], w2[6 * p + 2 * q, lanes])
                value = part[n, q] + term if p else part[n, q] - term
                for g in range(width // LANES):
                    wide[g, pl.ds(p * own * 2 + q, own, 2), :] = value[:, g * LANES : (g + 1) * LANES]
            for g in range(width // LANES):
                tile = wide[g, pl.ds(p * own * 2, own * 2), :].astype(BF16)
                out_ref[:, p, :, pl.ds(n * width + g * LANES, LANES)] = tile.reshape(rows, 2 * cols, LANES)

    pltpu.make_async_copy(stat_in, stat_in, stat_send).wait()

    @pl.when(has_up)
    def _():
        up_copy.wait_send()

    @pl.when(has_down)
    def _():
        down_copy.wait_send()


def per_device(n_view, latents, norm_gain, norm_shift, w_first, bias_first, w_second, bias_second):
    rows, cols, chans = latents.shape
    own = rows * cols
    flat = lambda w: jnp.transpose(w, (1, 2, 0, 3)).reshape(9, chans, chans)
    row = lambda v: v.reshape(1, chans)
    hbm = pl.BlockSpec(memory_space=pl.ANY)
    n_stat = 2 * chans // LANES
    out = pl.pallas_call(
        functools.partial(kernel, n_view, rows, cols, chans),
        out_shape=pltpu.VMEM((rows, 2, 2 * cols, chans), BF16),
        in_specs=[hbm] * 7,
        out_specs=pl.BlockSpec(memory_space=pltpu.VMEM),
        scratch_shapes=[
            pltpu.VMEM((rows + 4, cols, chans), BF16),
            pltpu.VMEM((4, 1, chans), F32),
            pltpu.VMEM((9, chans, chans), BF16),
            pltpu.VMEM((4, 3, chans, chans), BF16),
            pltpu.VMEM((9, chans, chans), BF16),
            pltpu.VMEM((5, chans, chans), BF16),
            pltpu.VMEM((3, rows + 4, cols, chans), BF16),
            pltpu.VMEM((4, 3, (rows // 2 + 1) * cols, chans), BF16),
            pltpu.VMEM((4, (rows // 2 + 1) * cols, chans), F32),
            pltpu.VMEM((3, rows + 2, cols, chans), BF16),
            pltpu.VMEM((3, own, chans), BF16),
            pltpu.VMEM((3, own + cols, chans), BF16),
            pltpu.VMEM((chans // TILE, 2, own, TILE), F32),
            pltpu.VMEM((TILE // LANES, own * 4, LANES), F32),
            pltpu.VMEM((n_stat, LANES), F32),
            pltpu.VMEM((n_view - 1, n_stat, LANES), F32),
            pltpu.SemaphoreType.DMA((rows,)),
            pltpu.SemaphoreType.DMA((4,)),
            pltpu.SemaphoreType.DMA((9,)),
            pltpu.SemaphoreType.DMA((9,)),
            pltpu.SemaphoreType.DMA((2,)),
            pltpu.SemaphoreType.DMA((2,)),
            pltpu.SemaphoreType.DMA,
            pltpu.SemaphoreType.DMA,
        ],
        compiler_params=pltpu.CompilerParams(
            collective_id=0, has_side_effects=True, vmem_limit_bytes=60 * 1024 * 1024
        ),
    )(
        latents, row(norm_gain), row(norm_shift), flat(w_first), row(bias_first), flat(w_second),
        row(bias_second),
    )
    return out.reshape(2 * rows, 2 * cols, chans)


def solution(mesh):
    placed = (P(("scene", "view"), None, None), P(), P(), P(), P(), P(), P())
    return jax.shard_map(
        functools.partial(per_device, mesh.shape["view"]),
        mesh=mesh,
        in_specs=placed,
        out_specs=P(("scene", "view"), None, None),
        check_vma=False,
    )
```

```python
import functools

import jax
import jax.numpy as jnp
from jax import lax
from jax.experimental import pallas as pl
from jax.experimental.pallas import tpu as pltpu
from jax.sharding import PartitionSpec as P

GROUPS = 32
H_LAT = 32
EPSILON = 1e-06
LANES = 128
TILE = 256
F32 = jnp.float32
BF16 = jnp.bfloat16


def dot_nt(x, w):
    return lax.dot_general(x, w, (((1,), (1,)), ((), ())), preferred_element_type=F32)


def dot_nn(x, w):
    return lax.dot_general(x, w, (((1,), (0,)), ((), ())), preferred_element_type=F32)


def kernel(
    n_view, rows, cols, chans,
    lat_hbm, gain_hbm, shift_hbm, w1_hbm, b1_hbm, w2_hbm, b2_hbm,
    out_ref,
    lat, small, w1, gt, w2, fold, act, vbuf, mbuf, mx, lhs_u, part, wide, stat, stat_in,
    lat_sem, small_sem, w1_sem, w2_sem, halo_send, halo_recv, stat_send, stat_recv,
):
    me = lax.axis_index("view")
    slabs = H_LAT // rows
    views = n_view // slabs
    slab = me // views
    own = rows * cols
    has_up = slab > 0
    has_down = slab < slabs - 1

    barrier = pltpu.get_barrier_semaphore()

    def greet(k, carry):
        pl.semaphore_signal(barrier, inc=1, device_id={"view": lax.rem(me + k, n_view)})
        return carry

    lat_rows = rows // 4

    def lat_copy(i):
        some = pl.ds(i * lat_rows, lat_rows)
        return pltpu.make_async_copy(lat_hbm.at[some], lat.at[pl.ds(2 + i * lat_rows, lat_rows)], lat_sem.at[i])

    def small_copy(i):
        ref = (gain_hbm, shift_hbm, b1_hbm, b2_hbm)[i]
        return pltpu.make_async_copy(ref, small.at[i], small_sem)

    def w1_copy(t):
        return pltpu.make_async_copy(w1_hbm.at[t], w1.at[t], w1_sem.at[t // 5])

    def w2_copy(t):
        return pltpu.make_async_copy(w2_hbm.at[t], w2.at[t], w2_sem)

    for i in range(4):
        lat_copy(i).start()
    lax.fori_loop(1, n_view, greet, 0, unroll=n_view <= 16)
    for t in range(9):
        w1_copy(t).start()
    for i in range(4):
        small_copy(i).start()

    tiles = chans // TILE
    eye = (
        lax.broadcasted_iota(jnp.int32, (TILE, TILE), 0) == lax.broadcasted_iota(jnp.int32, (TILE, TILE), 1)
    ).astype(F32).astype(BF16)

    def prepare(j, carry):
        k0 = pl.multiple_of(j // tiles * TILE, TILE)
        n0 = pl.multiple_of(lax.rem(j, tiles) * TILE, TILE)
        for s in range(3):
            for k, r in ((0, 0), (3, 2)):
                g = w1[3 * r + s, pl.ds(n0, TILE), pl.ds(k0, TILE)]
                gt[k, s, pl.ds(k0, TILE), pl.ds(n0, TILE)] = dot_nt(eye, g).astype(BF16)
            for a in range(0, TILE, LANES):
                for b in range(0, TILE, LANES):
                    n_at, k_at = pl.ds(n0 + a, LANES), pl.ds(k0 + b, LANES)
                    h = [w1[3 * r + s, n_at, k_at].astype(F32) for r in range(3)]
                    even = (h[0] + h[2]) * 0.5
                    odd = h[1] * 0.5
                    gt[1, s, k_at, n_at] = (even + odd).astype(BF16).T
                    gt[2, s, k_at, n_at] = (even - odd).astype(BF16).T
        return carry

    def prepare_all():
        pltpu.make_async_copy(w1.at[pl.ds(0, 5)], w1.at[pl.ds(0, 5)], w1_sem.at[0]).wait()
        for t in range(9):
            w2_copy(t).start()
        pltpu.make_async_copy(w1.at[pl.ds(5, 4)], w1.at[pl.ds(5, 4)], w1_sem.at[1]).wait()
        lax.fori_loop(0, tiles * tiles, prepare, 0)

    sums = jnp.zeros((8, chans), F32)
    squares = jnp.zeros((8, chans), F32)
    for i in range(rows):
        if i % lat_rows == 0:
            lat_copy(i // lat_rows).wait()
        x = lat[2 + i].astype(F32).reshape(cols // 8, 8, chans)
        sums = sums + jnp.sum(x, axis=0)
        squares = squares + jnp.sum(x * x, axis=0)
    sums = jnp.sum(sums, axis=0, keepdims=True)
    squares = jnp.sum(squares, axis=0, keepdims=True)
    blocks = chans // LANES
    stat[...] = jnp.concatenate(
        [v[:, k * LANES : (k + 1) * LANES] for v in (sums, squares) for k in range(blocks)], axis=0
    )

    @pl.when(jnp.logical_not(has_up))
    def _():
        prepare_all()

    pl.semaphore_wait(barrier, n_view - 1)

    def send_stat(k, carry):
        to = k + (k >= me).astype(jnp.int32)
        slot = lax.rem(to - me + n_view, n_view) - 1
        pltpu.make_async_remote_copy(
            src_ref=stat, dst_ref=stat_in.at[slot], send_sem=stat_send, recv_sem=stat_recv,
            device_id={"view": to},
        ).start()
        return carry

    lax.fori_loop(0, n_view - 1, send_stat, 0, unroll=n_view <= 16)

    up_copy = pltpu.make_async_remote_copy(
        src_ref=lat.at[pl.ds(2, 2)], dst_ref=lat.at[pl.ds(rows + 2, 2)],
        send_sem=halo_send.at[0], recv_sem=halo_recv.at[0],
        device_id={"view": jnp.maximum(me - views, 0)},
    )
    down_copy = pltpu.make_async_remote_copy(
        src_ref=lat.at[pl.ds(rows, 2)], dst_ref=lat.at[pl.ds(0, 2)],
        send_sem=halo_send.at[1], recv_sem=halo_recv.at[1],
        device_id={"view": jnp.minimum(me + views, n_view - 1)},
    )

    @pl.when(has_up)
    def _():
        up_copy.start()

    @pl.when(has_down)
    def _():
        down_copy.start()

    @pl.when(has_up)
    def _():
        prepare_all()

    pltpu.make_async_copy(w2, w2, w2_sem).wait()

    def fold_tile(j, carry):
        k0 = pl.multiple_of(j // tiles * TILE, TILE)
        n0 = pl.multiple_of(lax.rem(j, tiles) * TILE, TILE)
        for k, t in enumerate((0, 2, 6, 8)):
            g = w2[t, pl.ds(n0, TILE), pl.ds(k0, TILE)]
            fold[5 + k, pl.ds(k0, TILE), pl.ds(n0, TILE)] = dot_nt(eye, g).astype(BF16)
        for a in range(0, TILE, LANES):
            for b in range(0, TILE, LANES):
                n_at, k_at = pl.ds(n0 + a, LANES), pl.ds(k0 + b, LANES)

                def add(*taps):
                    terms = [w2[t, n_at, k_at].astype(F32) for t in taps]
                    return terms[0] + terms[1] + terms[2]

                def put(i, v):
                    fold[i, k_at, n_at] = v.astype(BF16).T

                put(3, add(0, 1, 2))
                put(4, add(6, 7, 8))
                left = add(0, 3, 6)
                put(1, left)
                right = add(2, 5, 8)
                put(2, right)
                put(0, left + add(1, 4, 7) + right)
        return carry

    lax.fori_loop(0, tiles * tiles, fold_tile, 0)
    pltpu.make_async_copy(small, small, small_sem).wait()

    same = (
        lax.broadcasted_iota(jnp.int32, (LANES, LANES), 0) // (chans // GROUPS)
        == lax.broadcasted_iota(jnp.int32, (LANES, LANES), 1) // (chans // GROUPS)
    ).astype(F32).astype(BF16)

    pltpu.make_async_copy(stat_in, stat_in, stat_recv).wait()

    total = stat[...] + jnp.sum(stat_in[...], axis=0)
    high = total.astype(BF16).astype(F32)
    rest = total - high
    middle = rest.astype(BF16).astype(F32)
    low = rest - middle
    parts = jnp.concatenate([high, middle, low, jnp.zeros_like(low)], axis=0).astype(BF16)
    sized = dot_nn(parts, same)
    n_stat = 2 * blocks
    total = sized[:n_stat] + sized[n_stat : 2 * n_stat] + sized[2 * n_stat : 3 * n_stat]
    entries = float(own * (chans // GROUPS) * n_view)
    mean = total[:blocks] / entries
    var = total[blocks:] / entries - mean * mean
    inv = lax.rsqrt(var + EPSILON)

    def one_row(v):
        return jnp.concatenate([v[k : k + 1] for k in range(blocks)], axis=1)

    scale = one_row(inv) * small[0]
    offset = small[1] - one_row(mean) * scale
    half_scale = scale * 0.5
    half_offset = offset * 0.5

    groups = range(chans // LANES)
    first_row = lax.broadcasted_iota(jnp.int32, (8, LANES), 0)

    def left_of(x):
        y = pltpu.roll(x, 1, 0)
        return jnp.concatenate([jnp.where(first_row == 0, 0.0, y[:8]), y[8:]], axis=0)

    def right_of(x):
        y = pltpu.roll(x, cols - 1, 0)
        return jnp.concatenate([y[:-8], jnp.where(first_row == 7, 0.0, y[-8:])], axis=0)

    def activate(i):
        for g in groups:
            lanes = pl.ds(g * LANES, LANES)
            side = slice(g * LANES, (g + 1) * LANES)
            h = lat[i, :, lanes].astype(F32) * half_scale[:, side] + half_offset[:, side]
            a = h + h * jnp.tanh(h)
            if i < 2:
                a = jnp.where(has_up, a, 0.0)
            if i >= rows + 2:
                a = jnp.where(has_down, a, 0.0)
            act[0, i, :, lanes] = left_of(a).astype(BF16)
            act[1, i, :, lanes] = a.astype(BF16)
            act[2, i, :, lanes] = right_of(a).astype(BF16)

    inner = list(range(1, rows // 2))
    outer = [0, rows // 2]
    place = {p: k for k, p in enumerate(inner + outer)}

    def arrange(k, pairs):
        a, b = ((0, 2), (1, 2), (2, 1), (1, 3))[k]
        for p in pairs:
            at = pl.ds(place[p] * cols, cols)
            for s in range(3):
                x, y = act[s, 2 * p + a], act[s, 2 * p + b]
                vbuf[k, s, at] = x + y if k == 1 else x - y

    def products(n, k, pairs):
        at = pl.ds(place[pairs[0]] * cols, len(pairs) * cols)
        lanes = pl.ds(n * TILE, TILE)
        terms = [dot_nn(vbuf[k, s, at], gt[k, s, :, lanes]) for s in range(3)]
        mbuf[k, at, lanes] = terms[0] + terms[1] + terms[2]

    bias1 = small[2]

    def mix(n, i):
        p, odd = i // 2, i % 2
        at = pl.ds(place[p] * cols, cols)
        for g in groups[n * TILE // LANES : (n + 1) * TILE // LANES]:
            lanes = pl.ds(g * LANES, LANES)
            v = [mbuf[k, at, lanes] for k in ((1, 2, 3) if odd else (0, 1, 2))]
            conv = v[0] - v[1] - v[2] if odd else v[0] + v[1] + v[2]
            m = lat[i + 1, :, lanes].astype(F32) + conv + bias1[:, g * LANES : (g + 1) * LANES]
            if i == 0:
                m = jnp.where(has_up, m, 0.0)
            if i == rows + 1:
                m = jnp.where(has_down, m, 0.0)
            narrow = m.astype(BF16)
            m = narrow.astype(F32)
            to = pl.ds(i * cols, cols)
            mx[0, to, lanes] = narrow
            mx[1, to, lanes] = left_of(m).astype(BF16) - narrow
            mx[2, to, lanes] = right_of(m).astype(BF16) - narrow

    def rise_of(n, j):
        lanes = pl.ds(n * TILE, TILE)
        here, below = pl.ds(j * cols, cols), pl.ds((j + 1) * cols, cols)
        for s in range(3):
            lhs_u[s, here, lanes] = mx[s, below, lanes] - mx[s, here, lanes]

    width = TILE
    bias2 = small[3]

    def take(ref, s, pieces):
        return jnp.concatenate([ref[s, pl.ds(a * cols, b * cols)] for a, b in pieces], axis=0)

    def level(n, pieces):
        lanes = pl.ds(n * width, width)
        mine = [(a + 1, b) for a, b in pieces]
        base = dot_nn(take(mx, 0, mine), fold[0, :, lanes]) + bias2[:, n * width : (n + 1) * width]
        for q in range(2):
            both = base + dot_nn(take(mx, 1 + q, mine), fold[1 + q, :, lanes])
            done = 0
            for a, b in pieces:
                part[n, q, pl.ds(a * cols, b * cols)] = both[done * cols : (done + b) * cols]
                done += b

    def finish(n, p, pieces):
        lanes = pl.ds(n * width, width)
        mine = [(a + p, b) for a, b in pieces]
        rise = dot_nn(take(lhs_u, 0, mine), fold[3 + p, :, lanes])
        for q in range(2):
            term = rise + dot_nn(take(lhs_u, 1 + q, mine), fold[5 + 2 * p + q, :, lanes])
            done = 0
            for a, b in pieces:
                for i in range(a, a + b):
                    for g in range(width // LANES):
                        x = part[n, q, pl.ds(i * cols, cols), pl.ds(g * LANES, LANES)]
                        y = term[done * cols : (done + 1) * cols, g * LANES : (g + 1) * LANES]
                        wide[g, pl.ds((p * rows + i) * 2 * cols + q, cols, 2), :] = x + y if p else x - y
                    done += 1
        for a, b in pieces:
            for i in range(a, a + b):
                for g in range(width // LANES):
                    tile = wide[g, pl.ds((p * rows + i) * 2 * cols, 2 * cols), :].astype(BF16)
                    out_ref[i, p, :, pl.ds(n * width + g * LANES, LANES)] = tile

    columns = range(chans // width)
    for i in range(2, rows + 2, 2):
        activate(i)
    arrange(0, inner)
    products(0, 0, inner)
    for i in range(3, rows + 2, 2):
        activate(i)
    for k in range(1, 4):
        arrange(k, inner)
        products(0, k, inner)
    for n in columns[1:]:
        for k in range(4):
            products(n, k, inner)
        for i in range(2, rows):
            mix(n - 1, i)
    for i in range(2, rows):
        mix(columns[-1], i)
    for n in columns:
        level(n, [(1, rows - 2)])
    for n in columns:
        for j in range(2, rows - 1):
            rise_of(n, j)

    @pl.when(has_up)
    def _():
        down_copy.wait_recv()

    @pl.when(has_down)
    def _():
        up_copy.wait_recv()

    for i in (0, 1, rows + 2, rows + 3):
        activate(i)
    for k in range(4):
        arrange(k, outer)
        products(0, k, outer)
    for n in columns[1:]:
        for k in range(4):
            products(n, k, outer)
        for i in (0, 1, rows, rows + 1):
            mix(n - 1, i)
    finish(0, 0, [(2, rows - 3)])
    for i in (0, 1, rows, rows + 1):
        mix(columns[-1], i)
    for n in columns:
        for j in (0, 1, rows - 1, rows):
            rise_of(n, j)
    for n in columns:
        level(n, [(0, 1), (rows - 1, 1)])
    finish(0, 0, [(0, 2), (rows - 1, 1)])
    finish(0, 1, [(0, rows)])
    for n in columns[1:]:
        finish(n, 0, [(0, rows)])
        for a in range(0, rows, rows // 4):
            finish(n, 1, [(a, rows // 4)])

    pltpu.make_async_copy(stat_in, stat_in, stat_send).wait()

    @pl.when(has_up)
    def _():
        up_copy.wait_send()

    @pl.when(has_down)
    def _():
        down_copy.wait_send()


def per_device(n_view, latents, norm_gain, norm_shift, w_first, bias_first, w_second, bias_second):
    rows, cols, chans = latents.shape
    own = rows * cols
    flat = lambda w: jnp.transpose(w, (1, 2, 0, 3)).reshape(9, chans, chans)
    row = lambda v: v.reshape(1, chans)
    hbm = pl.BlockSpec(memory_space=pl.ANY)
    n_stat = 2 * chans // LANES
    out = pl.pallas_call(
        functools.partial(kernel, n_view, rows, cols, chans),
        out_shape=pltpu.VMEM((rows, 2, 2 * cols, chans), BF16),
        in_specs=[hbm] * 7,
        out_specs=pl.BlockSpec(memory_space=pltpu.VMEM),
        scratch_shapes=[
            pltpu.VMEM((rows + 4, cols, chans), BF16),
            pltpu.VMEM((4, 1, chans), F32),
            pltpu.VMEM((9, chans, chans), BF16),
            pltpu.VMEM((4, 3, chans, chans), BF16),
            pltpu.VMEM((9, chans, chans), BF16),
            pltpu.VMEM((9, chans, chans), BF16),
            pltpu.VMEM((3, rows + 4, cols, chans), BF16),
            pltpu.VMEM((4, 3, (rows // 2 + 1) * cols, chans), BF16),
            pltpu.VMEM((4, (rows // 2 + 1) * cols, chans), F32),
            pltpu.VMEM((3, own + 2 * cols, chans), BF16),
            pltpu.VMEM((3, own + cols, chans), BF16),
            pltpu.VMEM((chans // TILE, 2, own, TILE), F32),
            pltpu.VMEM((TILE // LANES, own * 4, LANES), F32),
            pltpu.VMEM((n_stat, LANES), F32),
            pltpu.VMEM((n_view - 1, n_stat, LANES), F32),
            pltpu.SemaphoreType.DMA((4,)),
            pltpu.SemaphoreType.DMA,
            pltpu.SemaphoreType.DMA((2,)),
            pltpu.SemaphoreType.DMA,
            pltpu.SemaphoreType.DMA((2,)),
            pltpu.SemaphoreType.DMA((2,)),
            pltpu.SemaphoreType.DMA,
            pltpu.SemaphoreType.DMA,
        ],
        compiler_params=pltpu.CompilerParams(
            collective_id=0, has_side_effects=True, vmem_limit_bytes=60 * 1024 * 1024
        ),
    )(
        latents, row(norm_gain), row(norm_shift), flat(w_first), row(bias_first), flat(w_second),
        row(bias_second),
    )
    return out.reshape(2 * rows, 2 * cols, chans)


def solution(mesh):
    placed = (P(("scene", "view"), None, None), P(), P(), P(), P(), P(), P())
    return jax.shard_map(
        functools.partial(per_device, mesh.shape["view"]),
        mesh=mesh,
        in_specs=placed,
        out_specs=P(("scene", "view"), None, None),
        check_vma=False,
    )
```

```python
import functools

import jax
import jax.numpy as jnp
from jax import lax
from jax.experimental import pallas as pl
from jax.experimental.pallas import tpu as pltpu
from jax.sharding import PartitionSpec as P

GROUPS = 32
H_LAT = 32
EPSILON = 1e-06
LANES = 128
TILE = 256
F32 = jnp.float32
BF16 = jnp.bfloat16


def dot_nt(x, w):
    return lax.dot_general(x, w, (((1,), (1,)), ((), ())), preferred_element_type=F32)


def dot_nn(x, w):
    return lax.dot_general(x, w, (((1,), (0,)), ((), ())), preferred_element_type=F32)


def kernel(
    n_view, rows, cols, chans,
    lat_hbm, gain_hbm, shift_hbm, w1_hbm, b1_hbm, w2_hbm, b2_hbm,
    out_ref,
    lat, small, w1, gt, w2, fold, act, vbuf, mbuf, mx, lhs_u, part, wide, stat, stat_in,
    lat_sem, small_sem, w1_sem, w2_sem, halo_send, halo_recv, stat_send, stat_recv,
):
    me = lax.axis_index("view")
    slabs = H_LAT // rows
    views = n_view // slabs
    slab = me // views
    own = rows * cols
    has_up = slab > 0
    has_down = slab < slabs - 1

    barrier = pltpu.get_barrier_semaphore()

    def greet(k, carry):
        pl.semaphore_signal(barrier, inc=1, device_id={"view": lax.rem(me + k, n_view)})
        return carry

    lat_rows = rows // 4

    def lat_copy(i):
        some = pl.ds(i * lat_rows, lat_rows)
        return pltpu.make_async_copy(lat_hbm.at[some], lat.at[pl.ds(2 + i * lat_rows, lat_rows)], lat_sem.at[i])

    def small_copy(i):
        ref = (gain_hbm, shift_hbm, b1_hbm, b2_hbm)[i]
        return pltpu.make_async_copy(ref, small.at[i], small_sem)

    def w1_copy(t):
        return pltpu.make_async_copy(w1_hbm.at[t], w1.at[t], w1_sem.at[t // 5])

    def w2_copy(t):
        return pltpu.make_async_copy(w2_hbm.at[t], w2.at[t], w2_sem)

    for i in range(4):
        lat_copy(i).start()
    lax.fori_loop(1, n_view, greet, 0, unroll=n_view <= 16)
    for t in range(9):
        w1_copy(t).start()
    for i in range(4):
        small_copy(i).start()

    tiles = chans // TILE
    eye = (
        lax.broadcasted_iota(jnp.int32, (TILE, TILE), 0) == lax.broadcasted_iota(jnp.int32, (TILE, TILE), 1)
    ).astype(F32).astype(BF16)

    def prepare(j, carry):
        k0 = pl.multiple_of(j // tiles * TILE, TILE)
        n0 = pl.multiple_of(lax.rem(j, tiles) * TILE, TILE)
        for s in range(3):
            for k, r in ((0, 0), (3, 2)):
                g = w1[3 * r + s, pl.ds(n0, TILE), pl.ds(k0, TILE)]
                gt[k, s, pl.ds(k0, TILE), pl.ds(n0, TILE)] = dot_nt(eye, g).astype(BF16)
            for a in range(0, TILE, LANES):
                for b in range(0, TILE, LANES):
                    n_at, k_at = pl.ds(n0 + a, LANES), pl.ds(k0 + b, LANES)
                    h = [w1[3 * r + s, n_at, k_at].astype(F32) for r in range(3)]
                    even = (h[0] + h[2]) * 0.5
                    odd = h[1] * 0.5
                    gt[1, s, k_at, n_at] = (even + odd).astype(BF16).T
                    gt[2, s, k_at, n_at] = (even - odd).astype(BF16).T
        return carry

    def prepare_all():
        pltpu.make_async_copy(w1.at[pl.ds(0, 5)], w1.at[pl.ds(0, 5)], w1_sem.at[0]).wait()
        for t in range(9):
            w2_copy(t).start()
        pltpu.make_async_copy(w1.at[pl.ds(5, 4)], w1.at[pl.ds(5, 4)], w1_sem.at[1]).wait()
        lax.fori_loop(0, tiles * tiles, prepare, 0)

    sums = jnp.zeros((8, chans), F32)
    squares = jnp.zeros((8, chans), F32)
    for i in range(rows):
        if i % lat_rows == 0:
            lat_copy(i // lat_rows).wait()
        x = lat[2 + i].astype(F32).reshape(cols // 8, 8, chans)
        sums = sums + jnp.sum(x, axis=0)
        squares = squares + jnp.sum(x * x, axis=0)
    sums = jnp.sum(sums, axis=0, keepdims=True)
    squares = jnp.sum(squares, axis=0, keepdims=True)
    blocks = chans // LANES
    stat[...] = jnp.concatenate(
        [v[:, k * LANES : (k + 1) * LANES] for v in (sums, squares) for k in range(blocks)], axis=0
    )

    @pl.when(jnp.logical_not(has_up))
    def _():
        prepare_all()

    pl.semaphore_wait(barrier, n_view - 1)

    def send_stat(k, carry):
        to = k + (k >= me).astype(jnp.int32)
        slot = lax.rem(to - me + n_view, n_view) - 1
        pltpu.make_async_remote_copy(
            src_ref=stat, dst_ref=stat_in.at[slot], send_sem=stat_send, recv_sem=stat_recv,
            device_id={"view": to},
        ).start()
        return carry

    lax.fori_loop(0, n_view - 1, send_stat, 0, unroll=n_view <= 16)

    up_copy = pltpu.make_async_remote_copy(
        src_ref=lat.at[pl.ds(2, 2)], dst_ref=lat.at[pl.ds(rows + 2, 2)],
        send_sem=halo_send.at[0], recv_sem=halo_recv.at[0],
        device_id={"view": jnp.maximum(me - views, 0)},
    )
    down_copy = pltpu.make_async_remote_copy(
        src_ref=lat.at[pl.ds(rows, 2)], dst_ref=lat.at[pl.ds(0, 2)],
        send_sem=halo_send.at[1], recv_sem=halo_recv.at[1],
        device_id={"view": jnp.minimum(me + views, n_view - 1)},
    )

    own_up = pltpu.make_async_copy(lat_hbm.at[pl.ds(0, 2)], lat.at[pl.ds(0, 2)], halo_recv.at[1])
    own_down = pltpu.make_async_copy(lat_hbm.at[pl.ds(0, 2)], lat.at[pl.ds(rows + 2, 2)], halo_recv.at[0])

    @pl.when(has_up)
    def _():
        up_copy.start()

    @pl.when(jnp.logical_not(has_up))
    def _():
        own_up.start()

    @pl.when(has_down)
    def _():
        down_copy.start()

    @pl.when(jnp.logical_not(has_down))
    def _():
        own_down.start()

    @pl.when(has_up)
    def _():
        prepare_all()

    pltpu.make_async_copy(w2, w2, w2_sem).wait()

    def fold_tile(j, carry):
        k0 = pl.multiple_of(j // tiles * TILE, TILE)
        n0 = pl.multiple_of(lax.rem(j, tiles) * TILE, TILE)
        for k, t in enumerate((0, 2, 6, 8)):
            g = w2[t, pl.ds(n0, TILE), pl.ds(k0, TILE)]
            fold[5 + k, pl.ds(k0, TILE), pl.ds(n0, TILE)] = dot_nt(eye, g).astype(BF16)
        for a in range(0, TILE, LANES):
            for b in range(0, TILE, LANES):
                n_at, k_at = pl.ds(n0 + a, LANES), pl.ds(k0 + b, LANES)

                def add(*taps):
                    terms = [w2[t, n_at, k_at].astype(F32) for t in taps]
                    return terms[0] + terms[1] + terms[2]

                def put(i, v):
                    fold[i, k_at, n_at] = v.astype(BF16).T

                put(3, add(0, 1, 2))
                put(4, add(6, 7, 8))
                left = add(0, 3, 6)
                put(1, left)
                right = add(2, 5, 8)
                put(2, right)
                put(0, left + add(1, 4, 7) + right)
        return carry

    lax.fori_loop(0, tiles * tiles, fold_tile, 0)
    pltpu.make_async_copy(small, small, small_sem).wait()

    same = (
        lax.broadcasted_iota(jnp.int32, (LANES, LANES), 0) // (chans // GROUPS)
        == lax.broadcasted_iota(jnp.int32, (LANES, LANES), 1) // (chans // GROUPS)
    ).astype(F32).astype(BF16)

    pltpu.make_async_copy(stat_in, stat_in, stat_recv).wait()

    total = stat[...] + jnp.sum(stat_in[...], axis=0)
    high = total.astype(BF16).astype(F32)
    rest = total - high
    middle = rest.astype(BF16).astype(F32)
    low = rest - middle
    parts = jnp.concatenate([high, middle, low, jnp.zeros_like(low)], axis=0).astype(BF16)
    sized = dot_nn(parts, same)
    n_stat = 2 * blocks
    total = sized[:n_stat] + sized[n_stat : 2 * n_stat] + sized[2 * n_stat : 3 * n_stat]
    entries = float(own * (chans // GROUPS) * n_view)
    mean = total[:blocks] / entries
    var = total[blocks:] / entries - mean * mean
    inv = lax.rsqrt(var + EPSILON)

    def one_row(v):
        return jnp.concatenate([v[k : k + 1] for k in range(blocks)], axis=1)

    scale = one_row(inv) * small[0]
    offset = small[1] - one_row(mean) * scale
    half_scale = scale * 0.5
    half_offset = offset * 0.5

    groups = range(chans // LANES)
    first_row = lax.broadcasted_iota(jnp.int32, (8, LANES), 0)

    def left_of(x):
        y = pltpu.roll(x, 1, 0)
        return jnp.concatenate([jnp.where(first_row == 0, 0.0, y[:8]), y[8:]], axis=0)

    def right_of(x):
        y = pltpu.roll(x, cols - 1, 0)
        return jnp.concatenate([y[:-8], jnp.where(first_row == 7, 0.0, y[-8:])], axis=0)

    def activate(i):
        for g in groups:
            lanes = pl.ds(g * LANES, LANES)
            side = slice(g * LANES, (g + 1) * LANES)
            h = lat[i, :, lanes].astype(F32) * half_scale[:, side] + half_offset[:, side]
            a = h + h * jnp.tanh(h)
            if i < 2:
                a = jnp.where(has_up, a, 0.0)
            if i >= rows + 2:
                a = jnp.where(has_down, a, 0.0)
            act[0, i, :, lanes] = left_of(a).astype(BF16)
            act[1, i, :, lanes] = a.astype(BF16)
            act[2, i, :, lanes] = right_of(a).astype(BF16)

    inner = list(range(1, rows // 2))
    outer = [0, rows // 2]
    place = {p: k for k, p in enumerate(inner + outer)}

    def arrange(k, pairs):
        a, b = ((0, 2), (1, 2), (2, 1), (1, 3))[k]
        for p in pairs:
            at = pl.ds(place[p] * cols, cols)
            for s in range(3):
                x, y = act[s, 2 * p + a], act[s, 2 * p + b]
                vbuf[k, s, at] = x + y if k == 1 else x - y

    def products(n, k, pairs):
        at = pl.ds(place[pairs[0]] * cols, len(pairs) * cols)
        lanes = pl.ds(n * TILE, TILE)
        terms = [dot_nn(vbuf[k, s, at], gt[k, s, :, lanes]) for s in range(3)]
        mbuf[k, at, lanes] = terms[0] + terms[1] + terms[2]

    bias1 = small[2]

    def mix(n, i):
        p, odd = i // 2, i % 2
        at = pl.ds(place[p] * cols, cols)
        for g in groups[n * TILE // LANES : (n + 1) * TILE // LANES]:
            lanes = pl.ds(g * LANES, LANES)
            v = [mbuf[k, at, lanes] for k in ((1, 2, 3) if odd else (0, 1, 2))]
            conv = v[0] - v[1] - v[2] if odd else v[0] + v[1] + v[2]
            m = lat[i + 1, :, lanes].astype(F32) + conv + bias1[:, g * LANES : (g + 1) * LANES]
            if i == 0:
                m = jnp.where(has_up, m, 0.0)
            if i == rows + 1:
                m = jnp.where(has_down, m, 0.0)
            narrow = m.astype(BF16)
            m = narrow.astype(F32)
            to = pl.ds(i * cols, cols)
            mx[0, to, lanes] = narrow
            mx[1, to, lanes] = left_of(m).astype(BF16) - narrow
            mx[2, to, lanes] = right_of(m).astype(BF16) - narrow

    def rise_of(n, j):
        lanes = pl.ds(n * TILE, TILE)
        here, below = pl.ds(j * cols, cols), pl.ds((j + 1) * cols, cols)
        for s in range(3):
            lhs_u[s, here, lanes] = mx[s, below, lanes] - mx[s, here, lanes]

    width = TILE
    bias2 = small[3]

    def take(ref, s, pieces):
        return jnp.concatenate([ref[s, pl.ds(a * cols, b * cols)] for a, b in pieces], axis=0)

    def level(n, pieces):
        lanes = pl.ds(n * width, width)
        mine = [(a + 1, b) for a, b in pieces]
        base = dot_nn(take(mx, 0, mine), fold[0, :, lanes]) + bias2[:, n * width : (n + 1) * width]
        for q in range(2):
            both = base + dot_nn(take(mx, 1 + q, mine), fold[1 + q, :, lanes])
            done = 0
            for a, b in pieces:
                part[n, q, pl.ds(a * cols, b * cols)] = both[done * cols : (done + b) * cols]
                done += b

    def finish(n, p, pieces):
        lanes = pl.ds(n * width, width)
        mine = [(a + p, b) for a, b in pieces]
        rise = dot_nn(take(lhs_u, 0, mine), fold[3 + p, :, lanes])
        for q in range(2):
            term = rise + dot_nn(take(lhs_u, 1 + q, mine), fold[5 + 2 * p + q, :, lanes])
            done = 0
            for a, b in pieces:
                for i in range(a, a + b):
                    for g in range(width // LANES):
                        x = part[n, q, pl.ds(i * cols, cols), pl.ds(g * LANES, LANES)]
                        y = term[done * cols : (done + 1) * cols, g * LANES : (g + 1) * LANES]
                        wide[g, pl.ds((p * rows + i) * 2 * cols + q, cols, 2), :] = x + y if p else x - y
                    done += 1
        for a, b in pieces:
            for i in range(a, a + b):
                for g in range(width // LANES):
                    tile = wide[g, pl.ds((p * rows + i) * 2 * cols, 2 * cols), :].astype(BF16)
                    out_ref[i, p, :, pl.ds(n * width + g * LANES, LANES)] = tile

    columns = range(chans // width)

    for i in range(2, rows + 2, 2):
        activate(i)
    arrange(0, inner)
    for n in columns:
        products(n, 0, inner)
    for i in range(3, rows + 2, 2):
        activate(i)
    for n in columns:
        for k in range(1, 4):
            if n == 0:
                arrange(k, inner)
            products(n, k, inner)
        if n:
            for i in range(2, rows):
                mix(n - 1, i)
    for i in range(2, rows):
        mix(columns[-1], i)
    for n in columns:
        level(n, [(1, rows - 2)])
    for n in columns:
        for j in range(2, rows - 1):
            rise_of(n, j)

    own_up.wait()
    own_down.wait()
    for i in (0, rows + 2):
        activate(i)
    arrange(0, outer)
    for n in columns:
        products(n, 0, outer)
    for i in (1, rows + 3):
        activate(i)
    for n in columns:
        for k in range(1, 4):
            if n == 0:
                arrange(k, outer)
            products(n, k, outer)
        if n:
            for i in (0, 1, rows, rows + 1):
                mix(n - 1, i)
    finish(0, 0, [(2, rows - 3)])
    for i in (0, 1, rows, rows + 1):
        mix(columns[-1], i)
    for n in columns:
        for j in (0, 1, rows - 1, rows):
            rise_of(n, j)
    for n in columns:
        level(n, [(0, 1), (rows - 1, 1)])
    finish(0, 0, [(0, 2), (rows - 1, 1)])
    finish(0, 1, [(0, rows)])
    for n in columns[1:]:
        finish(n, 0, [(0, rows)])
        finish(n, 1, [(0, rows)])

    pltpu.make_async_copy(stat_in, stat_in, stat_send).wait()

    @pl.when(has_up)
    def _():
        up_copy.wait_send()

    @pl.when(has_down)
    def _():
        down_copy.wait_send()


def per_device(n_view, latents, norm_gain, norm_shift, w_first, bias_first, w_second, bias_second):
    rows, cols, chans = latents.shape
    own = rows * cols
    flat = lambda w: jnp.transpose(w, (1, 2, 0, 3)).reshape(9, chans, chans)
    row = lambda v: v.reshape(1, chans)
    hbm = pl.BlockSpec(memory_space=pl.ANY)
    n_stat = 2 * chans // LANES
    out = pl.pallas_call(
        functools.partial(kernel, n_view, rows, cols, chans),
        out_shape=pltpu.VMEM((rows, 2, 2 * cols, chans), BF16),
        in_specs=[hbm] * 7,
        out_specs=pl.BlockSpec(memory_space=pltpu.VMEM),
        scratch_shapes=[
            pltpu.VMEM((rows + 4, cols, chans), BF16),
            pltpu.VMEM((4, 1, chans), F32),
            pltpu.VMEM((9, chans, chans), BF16),
            pltpu.VMEM((4, 3, chans, chans), BF16),
            pltpu.VMEM((9, chans, chans), BF16),
            pltpu.VMEM((9, chans, chans), BF16),
            pltpu.VMEM((3, rows + 4, cols, chans), BF16),
            pltpu.VMEM((4, 3, (rows // 2 + 1) * cols, chans), BF16),
            pltpu.VMEM((4, (rows // 2 + 1) * cols, chans), F32),
            pltpu.VMEM((3, own + 2 * cols, chans), BF16),
            pltpu.VMEM((3, own + cols, chans), BF16),
            pltpu.VMEM((chans // TILE, 2, own, TILE), F32),
            pltpu.VMEM((TILE // LANES, own * 4, LANES), F32),
            pltpu.VMEM((n_stat, LANES), F32),
            pltpu.VMEM((n_view - 1, n_stat, LANES), F32),
            pltpu.SemaphoreType.DMA((4,)),
            pltpu.SemaphoreType.DMA,
            pltpu.SemaphoreType.DMA((2,)),
            pltpu.SemaphoreType.DMA,
            pltpu.SemaphoreType.DMA((2,)),
            pltpu.SemaphoreType.DMA((2,)),
            pltpu.SemaphoreType.DMA,
            pltpu.SemaphoreType.DMA,
        ],
        compiler_params=pltpu.CompilerParams(
            collective_id=0, has_side_effects=True, vmem_limit_bytes=60 * 1024 * 1024
        ),
    )(
        latents, row(norm_gain), row(norm_shift), flat(w_first), row(bias_first), flat(w_second),
        row(bias_second),
    )
    return out.reshape(2 * rows, 2 * cols, chans)


def solution(mesh):
    placed = (P(("scene", "view"), None, None), P(), P(), P(), P(), P(), P())
    return jax.shard_map(
        functools.partial(per_device, mesh.shape["view"]),
        mesh=mesh,
        in_specs=placed,
        out_specs=P(("scene", "view"), None, None),
        check_vma=False,
    )
```

```python
import functools

import jax
import jax.numpy as jnp
from jax import lax
from jax.experimental import pallas as pl
from jax.experimental.pallas import tpu as pltpu
from jax.sharding import PartitionSpec as P

GROUPS = 32
H_LAT = 32
EPSILON = 1e-06
LANES = 128
TILE = 256
F32 = jnp.float32
BF16 = jnp.bfloat16


def dot_nt(x, w):
    return lax.dot_general(x, w, (((1,), (1,)), ((), ())), preferred_element_type=F32)


def dot_nn(x, w):
    return lax.dot_general(x, w, (((1,), (0,)), ((), ())), preferred_element_type=F32)


def kernel(
    n_view, rows, cols, chans,
    lat_hbm, gain_hbm, shift_hbm, w1_hbm, b1_hbm, w2_hbm, b2_hbm,
    out_ref,
    lat, small, w1, gt, w2, fold, act, vbuf, mbuf, mx, lhs_u, part, wide, edge, stat, stat_in,
    lat_sem, small_sem, w1_sem, w2_sem, halo_send, halo_recv, stat_send, stat_recv,
):
    me = lax.axis_index("view")
    slabs = H_LAT // rows
    views = n_view // slabs
    slab = me // views
    own = rows * cols
    has_up = slab > 0
    has_down = slab < slabs - 1

    barrier = pltpu.get_barrier_semaphore()

    def greet(k, carry):
        pl.semaphore_signal(barrier, inc=1, device_id={"view": lax.rem(me + k, n_view)})
        return carry

    lat_rows = 1

    def lat_copy(i):
        some = pl.ds(i * lat_rows, lat_rows)
        return pltpu.make_async_copy(lat_hbm.at[some], lat.at[pl.ds(2 + i * lat_rows, lat_rows)], lat_sem.at[i])

    def small_copy(i):
        ref = (gain_hbm, shift_hbm, b1_hbm, b2_hbm)[i]
        return pltpu.make_async_copy(ref, small.at[i], small_sem)

    def w1_copy(t):
        return pltpu.make_async_copy(w1_hbm.at[t], w1.at[t], w1_sem.at[t // 5])

    def w2_copy(t):
        return pltpu.make_async_copy(w2_hbm.at[t], w2.at[t], w2_sem)

    for i in range(rows):
        lat_copy(i).start()
    lax.fori_loop(1, n_view, greet, 0, unroll=n_view <= 16)
    for t in range(9):
        w1_copy(t).start(priority=1)
    for i in range(4):
        small_copy(i).start(priority=1)

    tiles = chans // TILE
    eye = (
        lax.broadcasted_iota(jnp.int32, (TILE, TILE), 0) == lax.broadcasted_iota(jnp.int32, (TILE, TILE), 1)
    ).astype(F32).astype(BF16)

    def prepare(j, carry):
        k0 = pl.multiple_of(j // tiles * TILE, TILE)
        n0 = pl.multiple_of(lax.rem(j, tiles) * TILE, TILE)
        for s in range(3):
            for k, r in ((0, 0), (3, 2)):
                g = w1[3 * r + s, pl.ds(n0, TILE), pl.ds(k0, TILE)]
                gt[k, s, pl.ds(k0, TILE), pl.ds(n0, TILE)] = dot_nt(eye, g).astype(BF16)
            for a in range(0, TILE, LANES):
                for b in range(0, TILE, LANES):
                    n_at, k_at = pl.ds(n0 + a, LANES), pl.ds(k0 + b, LANES)
                    h = [w1[3 * r + s, n_at, k_at].astype(F32) for r in range(3)]
                    even = (h[0] + h[2]) * 0.5
                    odd = h[1] * 0.5
                    gt[1, s, k_at, n_at] = (even + odd).astype(BF16).T
                    gt[2, s, k_at, n_at] = (even - odd).astype(BF16).T
        return carry

    def prepare_all():
        pltpu.make_async_copy(w1.at[pl.ds(0, 5)], w1.at[pl.ds(0, 5)], w1_sem.at[0]).wait()
        for t in range(9):
            w2_copy(t).start(priority=1)
        pltpu.make_async_copy(w1.at[pl.ds(5, 4)], w1.at[pl.ds(5, 4)], w1_sem.at[1]).wait()
        lax.fori_loop(0, tiles * tiles, prepare, 0)

    sums = jnp.zeros((8, chans), F32)
    squares = jnp.zeros((8, chans), F32)
    for i in range(rows):
        if i % lat_rows == 0:
            lat_copy(i // lat_rows).wait()
        x = lat[2 + i].astype(F32).reshape(cols // 8, 8, chans)
        sums = sums + jnp.sum(x, axis=0)
        squares = squares + jnp.sum(x * x, axis=0)
    sums = jnp.sum(sums, axis=0, keepdims=True)
    squares = jnp.sum(squares, axis=0, keepdims=True)
    blocks = chans // LANES
    stat[...] = jnp.concatenate(
        [v[:, k * LANES : (k + 1) * LANES] for v in (sums, squares) for k in range(blocks)], axis=0
    )

    @pl.when(jnp.logical_not(has_up))
    def _():
        prepare_all()

    pl.semaphore_wait(barrier, n_view - 1)

    def send_stat(k, carry):
        to = k + (k >= me).astype(jnp.int32)
        slot = lax.rem(to - me + n_view, n_view) - 1
        pltpu.make_async_remote_copy(
            src_ref=stat, dst_ref=stat_in.at[slot], send_sem=stat_send, recv_sem=stat_recv,
            device_id={"view": to},
        ).start()
        return carry

    lax.fori_loop(0, n_view - 1, send_stat, 0, unroll=n_view <= 16)

    up_copy = pltpu.make_async_remote_copy(
        src_ref=lat.at[pl.ds(2, 2)], dst_ref=lat.at[pl.ds(rows + 2, 2)],
        send_sem=halo_send.at[0], recv_sem=halo_recv.at[0],
        device_id={"view": jnp.maximum(me - views, 0)},
    )
    down_copy = pltpu.make_async_remote_copy(
        src_ref=lat.at[pl.ds(rows, 2)], dst_ref=lat.at[pl.ds(0, 2)],
        send_sem=halo_send.at[1], recv_sem=halo_recv.at[1],
        device_id={"view": jnp.minimum(me + views, n_view - 1)},
    )

    own_up = pltpu.make_async_copy(lat_hbm.at[pl.ds(0, 2)], lat.at[pl.ds(0, 2)], halo_recv.at[1])
    own_down = pltpu.make_async_copy(lat_hbm.at[pl.ds(0, 2)], lat.at[pl.ds(rows + 2, 2)], halo_recv.at[0])

    @pl.when(has_up)
    def _():
        up_copy.start()

    @pl.when(jnp.logical_not(has_up))
    def _():
        own_up.start()

    @pl.when(has_down)
    def _():
        down_copy.start()

    @pl.when(jnp.logical_not(has_down))
    def _():
        own_down.start()

    @pl.when(has_up)
    def _():
        prepare_all()

    zeros = jnp.zeros((edge.shape[1], 8, LANES), F32)

    def clear(k, carry):
        edge[k, :, pl.ds(0, 8)] = zeros
        edge[k, :, pl.ds(cols + 8, 8)] = zeros
        return carry

    lax.fori_loop(0, edge.shape[0], clear, 0)
    pltpu.make_async_copy(w2, w2, w2_sem).wait()

    def fold_tile(j, carry):
        k0 = pl.multiple_of(j // tiles * TILE, TILE)
        n0 = pl.multiple_of(lax.rem(j, tiles) * TILE, TILE)
        for k, t in enumerate((0, 2, 6, 8)):
            g = w2[t, pl.ds(n0, TILE), pl.ds(k0, TILE)]
            fold[5 + k, pl.ds(k0, TILE), pl.ds(n0, TILE)] = dot_nt(eye, g).astype(BF16)
        for a in range(0, TILE, LANES):
            for b in range(0, TILE, LANES):
                n_at, k_at = pl.ds(n0 + a, LANES), pl.ds(k0 + b, LANES)

                def add(*taps):
                    terms = [w2[t, n_at, k_at].astype(F32) for t in taps]
                    return terms[0] + terms[1] + terms[2]

                def put(i, v):
                    fold[i, k_at, n_at] = v.astype(BF16).T

                put(3, add(0, 1, 2))
                put(4, add(6, 7, 8))
                left = add(0, 3, 6)
                put(1, left)
                right = add(2, 5, 8)
                put(2, right)
                put(0, left + add(1, 4, 7) + right)
        return carry

    lax.fori_loop(0, tiles * tiles, fold_tile, 0)
    pltpu.make_async_copy(small, small, small_sem).wait()

    same = (
        lax.broadcasted_iota(jnp.int32, (LANES, LANES), 0) // (chans // GROUPS)
        == lax.broadcasted_iota(jnp.int32, (LANES, LANES), 1) // (chans // GROUPS)
    ).astype(F32).astype(BF16)

    pltpu.make_async_copy(stat_in, stat_in, stat_recv).wait()

    total = stat[...] + jnp.sum(stat_in[...], axis=0)
    high = total.astype(BF16).astype(F32)
    rest = total - high
    middle = rest.astype(BF16).astype(F32)
    low = rest - middle
    parts = jnp.concatenate([high, middle, low, jnp.zeros_like(low)], axis=0).astype(BF16)
    sized = dot_nn(parts, same)
    n_stat = 2 * blocks
    total = sized[:n_stat] + sized[n_stat : 2 * n_stat] + sized[2 * n_stat : 3 * n_stat]
    entries = float(own * (chans // GROUPS) * n_view)
    mean = total[:blocks] / entries
    var = total[blocks:] / entries - mean * mean
    inv = lax.rsqrt(var + EPSILON)

    def one_row(v):
        return jnp.concatenate([v[k : k + 1] for k in range(blocks)], axis=1)

    scale = one_row(inv) * small[0]
    offset = small[1] - one_row(mean) * scale
    half_scale = scale * 0.5
    half_offset = offset * 0.5

    groups = range(chans // LANES)

    def beside(slot, g, x):
        edge[slot, g, pl.ds(8, cols)] = x
        return edge[slot, g, pl.ds(7, cols)], edge[slot, g, pl.ds(9, cols)]

    def activate(i):
        for g in groups:
            lanes = pl.ds(g * LANES, LANES)
            side = slice(g * LANES, (g + 1) * LANES)
            h = lat[i, :, lanes].astype(F32) * half_scale[:, side] + half_offset[:, side]
            a = h + h * jnp.tanh(h)
            if i < 2:
                a = jnp.where(has_up, a, 0.0)
            if i >= rows + 2:
                a = jnp.where(has_down, a, 0.0)
            left, right = beside(i, g, a)
            act[0, i, :, lanes] = left.astype(BF16)
            act[1, i, :, lanes] = a.astype(BF16)
            act[2, i, :, lanes] = right.astype(BF16)

    inner = list(range(1, rows // 2))
    outer = [0, rows // 2]
    place = {p: k for k, p in enumerate(inner + outer)}

    def arrange(k, pairs):
        a, b = ((0, 2), (1, 2), (2, 1), (1, 3))[k]
        for p in pairs:
            at = pl.ds(place[p] * cols, cols)
            for s in range(3):
                x, y = act[s, 2 * p + a], act[s, 2 * p + b]
                vbuf[k, s, at] = x + y if k == 1 else x - y

    def products(n, k, pairs):
        at = pl.ds(place[pairs[0]] * cols, len(pairs) * cols)
        lanes = pl.ds(n * TILE, TILE)
        terms = [dot_nn(vbuf[k, s, at], gt[k, s, :, lanes]) for s in range(3)]
        mbuf[k, at, lanes] = terms[0] + terms[1] + terms[2]

    bias1 = small[2]

    def mix(n, i):
        p, odd = i // 2, i % 2
        at = pl.ds(place[p] * cols, cols)
        for g in groups[n * TILE // LANES : (n + 1) * TILE // LANES]:
            lanes = pl.ds(g * LANES, LANES)
            v = [mbuf[k, at, lanes] for k in ((1, 2, 3) if odd else (0, 1, 2))]
            conv = v[0] - v[1] - v[2] if odd else v[0] + v[1] + v[2]
            m = lat[i + 1, :, lanes].astype(F32) + conv + bias1[:, g * LANES : (g + 1) * LANES]
            if i == 0:
                m = jnp.where(has_up, m, 0.0)
            if i == rows + 1:
                m = jnp.where(has_down, m, 0.0)
            narrow = m.astype(BF16)
            m = narrow.astype(F32)
            to = pl.ds(i * cols, cols)
            left, right = beside(rows + 4 + i, g, m)
            mx[0, to, lanes] = narrow
            mx[1, to, lanes] = left.astype(BF16) - narrow
            mx[2, to, lanes] = right.astype(BF16) - narrow

    def rise_of(n, j):
        lanes = pl.ds(n * TILE, TILE)
        here, below = pl.ds(j * cols, cols), pl.ds((j + 1) * cols, cols)
        for s in range(3):
            lhs_u[s, here, lanes] = mx[s, below, lanes] - mx[s, here, lanes]

    width = TILE
    bias2 = small[3]

    def take(ref, s, pieces):
        return jnp.concatenate([ref[s, pl.ds(a * cols, b * cols)] for a, b in pieces], axis=0)

    def level(n, pieces):
        lanes = pl.ds(n * width, width)
        mine = [(a + 1, b) for a, b in pieces]
        base = dot_nn(take(mx, 0, mine), fold[0, :, lanes]) + bias2[:, n * width : (n + 1) * width]
        for q in range(2):
            both = base + dot_nn(take(mx, 1 + q, mine), fold[1 + q, :, lanes])
            done = 0
            for a, b in pieces:
                part[n, q, pl.ds(a * cols, b * cols)] = both[done * cols : (done + b) * cols]
                done += b

    def finish(n, p, pieces):
        lanes = pl.ds(n * width, width)
        mine = [(a + p, b) for a, b in pieces]
        rise = dot_nn(take(lhs_u, 0, mine), fold[3 + p, :, lanes])
        for q in range(2):
            term = rise + dot_nn(take(lhs_u, 1 + q, mine), fold[5 + 2 * p + q, :, lanes])
            done = 0
            for a, b in pieces:
                for i in range(a, a + b):
                    for g in range(width // LANES):
                        x = part[n, q, pl.ds(i * cols, cols), pl.ds(g * LANES, LANES)]
                        y = term[done * cols : (done + 1) * cols, g * LANES : (g + 1) * LANES]
                        wide[g, pl.ds((p * rows + i) * 2 * cols + q, cols, 2), :] = x + y if p else x - y
                    done += 1
        for a, b in pieces:
            for i in range(a, a + b):
                for g in range(width // LANES):
                    tile = wide[g, pl.ds((p * rows + i) * 2 * cols, 2 * cols), :].astype(BF16)
                    out_ref[i, p, :, pl.ds(n * width + g * LANES, LANES)] = tile

    columns = range(chans // width)

    for i in range(2, rows + 2, 2):
        activate(i)
    arrange(0, inner)
    for n in columns:
        products(n, 0, inner)
    for i in range(3, rows + 2, 2):
        activate(i)
    for n in columns:
        for k in range(1, 4):
            if n == 0:
                arrange(k, inner)
            products(n, k, inner)
        if n:
            for i in range(2, rows):
                mix(n - 1, i)
    for i in range(2, rows):
        mix(columns[-1], i)
    for n in columns:
        level(n, [(1, rows - 2)])
    for n in columns:
        for j in range(2, rows - 1):
            rise_of(n, j)

    own_up.wait()
    own_down.wait()
    for i in (0, rows + 2):
        activate(i)
    arrange(0, outer)
    for n in columns:
        products(n, 0, outer)
    for i in (1, rows + 3):
        activate(i)
    for n in columns:
        for k in range(1, 4):
            if n == 0:
                arrange(k, outer)
            products(n, k, outer)
        if n:
            for i in (0, 1, rows, rows + 1):
                mix(n - 1, i)
    finish(0, 0, [(2, rows - 3)])
    for i in (0, 1, rows, rows + 1):
        mix(columns[-1], i)
    for n in columns:
        for j in (0, 1, rows - 1, rows):
            rise_of(n, j)
    for n in columns:
        level(n, [(0, 1), (rows - 1, 1)])
    finish(0, 0, [(0, 2), (rows - 1, 1)])
    finish(0, 1, [(0, rows)])
    for n in columns[1:]:
        finish(n, 0, [(0, rows)])
        finish(n, 1, [(0, rows)])

    pltpu.make_async_copy(stat_in, stat_in, stat_send).wait()

    @pl.when(has_up)
    def _():
        up_copy.wait_send()

    @pl.when(has_down)
    def _():
        down_copy.wait_send()


def per_device(n_view, latents, norm_gain, norm_shift, w_first, bias_first, w_second, bias_second):
    rows, cols, chans = latents.shape
    own = rows * cols
    flat = lambda w: jnp.transpose(w, (1, 2, 0, 3)).reshape(9, chans, chans)
    row = lambda v: v.reshape(1, chans)
    hbm = pl.BlockSpec(memory_space=pl.ANY)
    n_stat = 2 * chans // LANES
    out = pl.pallas_call(
        functools.partial(kernel, n_view, rows, cols, chans),
        out_shape=pltpu.VMEM((rows, 2, 2 * cols, chans), BF16),
        in_specs=[hbm] * 7,
        out_specs=pl.BlockSpec(memory_space=pltpu.VMEM),
        scratch_shapes=[
            pltpu.VMEM((rows + 4, cols, chans), BF16),
            pltpu.VMEM((4, 1, chans), F32),
            pltpu.VMEM((9, chans, chans), BF16),
            pltpu.VMEM((4, 3, chans, chans), BF16),
            pltpu.VMEM((9, chans, chans), BF16),
            pltpu.VMEM((9, chans, chans), BF16),
            pltpu.VMEM((3, rows + 4, cols, chans), BF16),
            pltpu.VMEM((4, 3, (rows // 2 + 1) * cols, chans), BF16),
            pltpu.VMEM((4, (rows // 2 + 1) * cols, chans), F32),
            pltpu.VMEM((3, own + 2 * cols, chans), BF16),
            pltpu.VMEM((3, own + cols, chans), BF16),
            pltpu.VMEM((chans // TILE, 2, own, TILE), F32),
            pltpu.VMEM((TILE // LANES, own * 4, LANES), F32),
            pltpu.VMEM((2 * rows + 6, chans // LANES, cols + 16, LANES), F32),
            pltpu.VMEM((n_stat, LANES), F32),
            pltpu.VMEM((n_view - 1, n_stat, LANES), F32),
            pltpu.SemaphoreType.DMA((rows,)),
            pltpu.SemaphoreType.DMA,
            pltpu.SemaphoreType.DMA((2,)),
            pltpu.SemaphoreType.DMA,
            pltpu.SemaphoreType.DMA((2,)),
            pltpu.SemaphoreType.DMA((2,)),
            pltpu.SemaphoreType.DMA,
            pltpu.SemaphoreType.DMA,
        ],
        compiler_params=pltpu.CompilerParams(
            collective_id=0, has_side_effects=True, vmem_limit_bytes=60 * 1024 * 1024
        ),
    )(
        latents, row(norm_gain), row(norm_shift), flat(w_first), row(bias_first), flat(w_second),
        row(bias_second),
    )
    return out.reshape(2 * rows, 2 * cols, chans)


def solution(mesh):
    placed = (P(("scene", "view"), None, None), P(), P(), P(), P(), P(), P())
    return jax.shard_map(
        functools.partial(per_device, mesh.shape["view"]),
        mesh=mesh,
        in_specs=placed,
        out_specs=P(("scene", "view"), None, None),
        check_vma=False,
    )
```

```python
import functools

import jax
import jax.numpy as jnp
from jax import lax
from jax.experimental import pallas as pl
from jax.experimental.pallas import tpu as pltpu
from jax.sharding import PartitionSpec as P

GROUPS = 32
H_LAT = 32
EPSILON = 1e-06
LANES = 128
TILE = 256
F32 = jnp.float32
BF16 = jnp.bfloat16


def dot_nt(x, w):
    return lax.dot_general(x, w, (((1,), (1,)), ((), ())), preferred_element_type=F32)


def dot_nn(x, w):
    return lax.dot_general(x, w, (((1,), (0,)), ((), ())), preferred_element_type=F32)


def kernel(
    n_view, rows, cols, chans,
    lat_hbm, gain_hbm, shift_hbm, w1_hbm, b1_hbm, w2_hbm, b2_hbm,
    out_ref,
    lat, small, w1, gt, w2, fold, act, vbuf, mbuf, mx, lhs_u, part, wide, edge, stat, stat_in,
    lat_sem, small_sem, w1_sem, w2_sem, halo_send, halo_recv, stat_send, stat_recv,
):
    me = lax.axis_index("view")
    slabs = H_LAT // rows
    views = n_view // slabs
    slab = me // views
    own = rows * cols
    has_up = slab > 0
    has_down = slab < slabs - 1

    barrier = pltpu.get_barrier_semaphore()

    def greet(k, carry):
        pl.semaphore_signal(barrier, inc=1, device_id={"view": lax.rem(me + k, n_view)})
        return carry

    lat_rows = 1

    def lat_copy(i):
        some = pl.ds(i * lat_rows, lat_rows)
        return pltpu.make_async_copy(lat_hbm.at[some], lat.at[pl.ds(2 + i * lat_rows, lat_rows)], lat_sem.at[i])

    def small_copy(i):
        ref = (gain_hbm, shift_hbm, b1_hbm, b2_hbm)[i]
        return pltpu.make_async_copy(ref, small.at[i], small_sem)

    def w1_copy(t):
        return pltpu.make_async_copy(w1_hbm.at[t], w1.at[t], w1_sem.at[t // 5])

    def w2_copy(t):
        return pltpu.make_async_copy(w2_hbm.at[t], w2.at[t], w2_sem)

    for i in range(rows):
        lat_copy(i).start()
    lax.fori_loop(1, n_view, greet, 0, unroll=n_view <= 16)
    for t in range(9):
        w1_copy(t).start(priority=1)
    for i in range(4):
        small_copy(i).start(priority=1)

    tiles = chans // TILE
    eye = (
        lax.broadcasted_iota(jnp.int32, (TILE, TILE), 0) == lax.broadcasted_iota(jnp.int32, (TILE, TILE), 1)
    ).astype(F32).astype(BF16)

    def prepare(j, carry):
        k0 = pl.multiple_of(j // tiles * TILE, TILE)
        n0 = pl.multiple_of(lax.rem(j, tiles) * TILE, TILE)
        for s in range(3):
            for k, r in ((0, 0), (3, 2)):
                g = w1[3 * r + s, pl.ds(n0, TILE), pl.ds(k0, TILE)]
                gt[k, s, pl.ds(k0, TILE), pl.ds(n0, TILE)] = dot_nt(eye, g).astype(BF16)
            for a in range(0, TILE, LANES):
                for b in range(0, TILE, LANES):
                    n_at, k_at = pl.ds(n0 + a, LANES), pl.ds(k0 + b, LANES)
                    h = [w1[3 * r + s, n_at, k_at].astype(F32) for r in range(3)]
                    even = (h[0] + h[2]) * 0.5
                    odd = h[1] * 0.5
                    gt[1, s, k_at, n_at] = (even + odd).astype(BF16).T
                    gt[2, s, k_at, n_at] = (even - odd).astype(BF16).T
        return carry

    def prepare_all():
        pltpu.make_async_copy(w1.at[pl.ds(0, 5)], w1.at[pl.ds(0, 5)], w1_sem.at[0]).wait()
        for t in range(9):
            w2_copy(t).start(priority=1)
        pltpu.make_async_copy(w1.at[pl.ds(5, 4)], w1.at[pl.ds(5, 4)], w1_sem.at[1]).wait()
        lax.fori_loop(0, tiles * tiles, prepare, 0)

    sums = jnp.zeros((8, chans), F32)
    squares = jnp.zeros((8, chans), F32)
    for i in range(rows):
        if i % lat_rows == 0:
            lat_copy(i // lat_rows).wait()
        x = lat[2 + i].astype(F32).reshape(cols // 8, 8, chans)
        sums = sums + jnp.sum(x, axis=0)
        squares = squares + jnp.sum(x * x, axis=0)
    sums = jnp.sum(sums, axis=0, keepdims=True)
    squares = jnp.sum(squares, axis=0, keepdims=True)
    blocks = chans // LANES
    stat[...] = jnp.concatenate(
        [v[:, k * LANES : (k + 1) * LANES] for v in (sums, squares) for k in range(blocks)], axis=0
    )

    @pl.when(jnp.logical_not(has_up))
    def _():
        prepare_all()

    pl.semaphore_wait(barrier, n_view - 1)

    def send_stat(k, carry):
        to = k + (k >= me).astype(jnp.int32)
        slot = lax.rem(to - me + n_view, n_view) - 1
        pltpu.make_async_remote_copy(
            src_ref=stat, dst_ref=stat_in.at[slot], send_sem=stat_send, recv_sem=stat_recv,
            device_id={"view": to},
        ).start()
        return carry

    lax.fori_loop(0, n_view - 1, send_stat, 0, unroll=n_view <= 16)

    up_copy = pltpu.make_async_remote_copy(
        src_ref=lat.at[pl.ds(2, 2)], dst_ref=lat.at[pl.ds(rows + 2, 2)],
        send_sem=halo_send.at[0], recv_sem=halo_recv.at[0],
        device_id={"view": jnp.maximum(me - views, 0)},
    )
    down_copy = pltpu.make_async_remote_copy(
        src_ref=lat.at[pl.ds(rows, 2)], dst_ref=lat.at[pl.ds(0, 2)],
        send_sem=halo_send.at[1], recv_sem=halo_recv.at[1],
        device_id={"view": jnp.minimum(me + views, n_view - 1)},
    )

    own_up = pltpu.make_async_copy(lat_hbm.at[pl.ds(0, 2)], lat.at[pl.ds(0, 2)], halo_recv.at[1])
    own_down = pltpu.make_async_copy(lat_hbm.at[pl.ds(0, 2)], lat.at[pl.ds(rows + 2, 2)], halo_recv.at[0])

    @pl.when(has_up)
    def _():
        up_copy.start()

    @pl.when(jnp.logical_not(has_up))
    def _():
        own_up.start()

    @pl.when(has_down)
    def _():
        down_copy.start()

    @pl.when(jnp.logical_not(has_down))
    def _():
        own_down.start()

    @pl.when(has_up)
    def _():
        prepare_all()

    zeros = jnp.zeros((edge.shape[1], 8, LANES), F32)

    def clear(k, carry):
        edge[k, :, pl.ds(0, 8)] = zeros
        edge[k, :, pl.ds(cols + 8, 8)] = zeros
        return carry

    lax.fori_loop(0, edge.shape[0], clear, 0)
    pltpu.make_async_copy(w2, w2, w2_sem).wait()

    def fold_tile(j, carry):
        k0 = pl.multiple_of(j // tiles * TILE, TILE)
        n0 = pl.multiple_of(lax.rem(j, tiles) * TILE, TILE)
        for k, t in enumerate((0, 2, 6, 8)):
            g = w2[t, pl.ds(n0, TILE), pl.ds(k0, TILE)]
            fold[5 + k, pl.ds(k0, TILE), pl.ds(n0, TILE)] = dot_nt(eye, g).astype(BF16)
        for a in range(0, TILE, LANES):
            for b in range(0, TILE, LANES):
                n_at, k_at = pl.ds(n0 + a, LANES), pl.ds(k0 + b, LANES)

                def add(*taps):
                    terms = [w2[t, n_at, k_at].astype(F32) for t in taps]
                    return terms[0] + terms[1] + terms[2]

                def put(i, v):
                    fold[i, k_at, n_at] = v.astype(BF16).T

                put(3, add(0, 1, 2))
                put(4, add(6, 7, 8))
                left = add(0, 3, 6)
                put(1, left)
                right = add(2, 5, 8)
                put(2, right)
                put(0, left + add(1, 4, 7) + right)
        return carry

    lax.fori_loop(0, tiles * tiles, fold_tile, 0)
    pltpu.make_async_copy(small, small, small_sem).wait()

    same = (
        lax.broadcasted_iota(jnp.int32, (LANES, LANES), 0) // (chans // GROUPS)
        == lax.broadcasted_iota(jnp.int32, (LANES, LANES), 1) // (chans // GROUPS)
    ).astype(F32).astype(BF16)

    pltpu.make_async_copy(stat_in, stat_in, stat_recv).wait()

    total = stat[...] + jnp.sum(stat_in[...], axis=0)
    high = total.astype(BF16).astype(F32)
    rest = total - high
    middle = rest.astype(BF16).astype(F32)
    low = rest - middle
    parts = jnp.concatenate([high, middle, low, jnp.zeros_like(low)], axis=0).astype(BF16)
    sized = dot_nn(parts, same)
    n_stat = 2 * blocks
    total = sized[:n_stat] + sized[n_stat : 2 * n_stat] + sized[2 * n_stat : 3 * n_stat]
    entries = float(own * (chans // GROUPS) * n_view)
    mean = total[:blocks] / entries
    var = total[blocks:] / entries - mean * mean
    inv = lax.rsqrt(var + EPSILON)

    def one_row(v):
        return jnp.concatenate([v[k : k + 1] for k in range(blocks)], axis=1)

    scale = one_row(inv) * small[0]
    offset = small[1] - one_row(mean) * scale
    half_scale = scale * 0.5
    half_offset = offset * 0.5

    groups = range(chans // LANES)

    def beside(slot, g, x):
        edge[slot, g, pl.ds(8, cols)] = x
        return edge[slot, g, pl.ds(7, cols)], edge[slot, g, pl.ds(9, cols)]

    def activate(i):
        for g in groups:
            lanes = pl.ds(g * LANES, LANES)
            side = slice(g * LANES, (g + 1) * LANES)
            h = lat[i, :, lanes].astype(F32) * half_scale[:, side] + half_offset[:, side]
            a = h + h * jnp.tanh(h)
            if i < 2:
                a = jnp.where(has_up, a, 0.0)
            if i >= rows + 2:
                a = jnp.where(has_down, a, 0.0)
            left, right = beside(i, g, a)
            act[0, i, :, lanes] = left.astype(BF16)
            act[1, i, :, lanes] = a.astype(BF16)
            act[2, i, :, lanes] = right.astype(BF16)

    inner = list(range(1, rows // 2))
    outer = [0, rows // 2]
    place = {p: k for k, p in enumerate(inner + outer)}

    def arrange(k, pairs):
        a, b = ((0, 2), (1, 2), (2, 1), (1, 3))[k]
        for p in pairs:
            at = pl.ds(place[p] * cols, cols)
            for s in range(3):
                x, y = act[s, 2 * p + a], act[s, 2 * p + b]
                vbuf[k, s, at] = x + y if k == 1 else x - y

    def products(n, k, pairs):
        at = pl.ds(place[pairs[0]] * cols, len(pairs) * cols)
        lanes = pl.ds(n * TILE, TILE)
        terms = [dot_nn(vbuf[k, s, at], gt[k, s, :, lanes]) for s in range(3)]
        mbuf[k, at, lanes] = terms[0] + terms[1] + terms[2]

    bias1 = small[2]

    def mix(n, i):
        p, odd = i // 2, i % 2
        at = pl.ds(place[p] * cols, cols)
        for g in groups[n * TILE // LANES : (n + 1) * TILE // LANES]:
            lanes = pl.ds(g * LANES, LANES)
            v = [mbuf[k, at, lanes] for k in ((1, 2, 3) if odd else (0, 1, 2))]
            conv = v[0] - v[1] - v[2] if odd else v[0] + v[1] + v[2]
            m = lat[i + 1, :, lanes].astype(F32) + conv + bias1[:, g * LANES : (g + 1) * LANES]
            if i == 0:
                m = jnp.where(has_up, m, 0.0)
            if i == rows + 1:
                m = jnp.where(has_down, m, 0.0)
            narrow = m.astype(BF16)
            m = narrow.astype(F32)
            to = pl.ds(i * cols, cols)
            left, right = beside(rows + 4 + i, g, m)
            mx[0, to, lanes] = narrow
            mx[1, to, lanes] = left.astype(BF16) - narrow
            mx[2, to, lanes] = right.astype(BF16) - narrow

    def rise_of(n, j):
        lanes = pl.ds(n * TILE, TILE)
        here, below = pl.ds(j * cols, cols), pl.ds((j + 1) * cols, cols)
        for s in range(3):
            lhs_u[s, here, lanes] = mx[s, below, lanes] - mx[s, here, lanes]

    width = TILE
    bias2 = small[3]

    def take(ref, s, pieces):
        return jnp.concatenate([ref[s, pl.ds(a * cols, b * cols)] for a, b in pieces], axis=0)

    def level(n, pieces):
        lanes = pl.ds(n * width, width)
        mine = [(a + 1, b) for a, b in pieces]
        base = dot_nn(take(mx, 0, mine), fold[0, :, lanes]) + bias2[:, n * width : (n + 1) * width]
        for q in range(2):
            both = base + dot_nn(take(mx, 1 + q, mine), fold[1 + q, :, lanes])
            done = 0
            for a, b in pieces:
                part[n, q, pl.ds(a * cols, b * cols)] = both[done * cols : (done + b) * cols]
                done += b

    def finish(n, p, pieces):
        lanes = pl.ds(n * width, width)
        mine = [(a + p, b) for a, b in pieces]
        rise = dot_nn(take(lhs_u, 0, mine), fold[3 + p, :, lanes])
        for q in range(2):
            term = rise + dot_nn(take(lhs_u, 1 + q, mine), fold[5 + 2 * p + q, :, lanes])
            done = 0
            for a, b in pieces:
                for i in range(a, a + b):
                    for g in range(width // LANES):
                        x = part[n, q, pl.ds(i * cols, cols), pl.ds(g * LANES, LANES)]
                        y = term[done * cols : (done + 1) * cols, g * LANES : (g + 1) * LANES]
                        wide[g, pl.ds((p * rows + i) * 2 * cols + q, cols, 2), :] = x + y if p else x - y
                    done += 1
        for a, b in pieces:
            for i in range(a, a + b):
                for g in range(width // LANES):
                    tile = wide[g, pl.ds((p * rows + i) * 2 * cols, 2 * cols), :].astype(BF16)
                    out_ref[i, p, :, pl.ds(n * width + g * LANES, LANES)] = tile

    columns = range(chans // width)

    for i in range(2, rows + 2, 2):
        activate(i)
    arrange(0, inner)
    for n in columns:
        products(n, 0, inner)
    for i in range(3, rows + 2, 2):
        activate(i)
    for n in columns:
        for k in range(1, 4):
            if n == 0:
                arrange(k, inner)
            products(n, k, inner)
        if n:
            for i in range(2, rows):
                mix(n - 1, i)
    for i in range(2, rows):
        mix(columns[-1], i)
    for n in columns:
        level(n, [(1, rows - 2)])
    for n in columns:
        for j in range(2, rows - 1):
            rise_of(n, j)

    own_up.wait()
    own_down.wait()
    finish(0, 0, [(2, rows - 3)])
    for i in (0, rows + 2):
        activate(i)
    arrange(0, outer)
    for n in columns:
        products(n, 0, outer)
    for i in (1, rows + 3):
        activate(i)
    for n in columns:
        for k in range(1, 4):
            if n == 0:
                arrange(k, outer)
            products(n, k, outer)
        if n:
            for i in (0, 1, rows, rows + 1):
                mix(n - 1, i)
    finish(0, 1, [(1, rows - 3)])
    for i in (0, 1, rows, rows + 1):
        mix(columns[-1], i)
    for n in columns:
        for j in (0, 1, rows - 1, rows):
            rise_of(n, j)
    for n in columns:
        level(n, [(0, 1), (rows - 1, 1)])
    finish(0, 0, [(0, 2), (rows - 1, 1)])
    finish(0, 1, [(0, 1), (rows - 2, 2)])
    for n in columns[1:]:
        finish(n, 0, [(0, rows)])
        finish(n, 1, [(0, rows)])

    pltpu.make_async_copy(stat_in, stat_in, stat_send).wait()

    @pl.when(has_up)
    def _():
        up_copy.wait_send()

    @pl.when(has_down)
    def _():
        down_copy.wait_send()


def per_device(n_view, latents, norm_gain, norm_shift, w_first, bias_first, w_second, bias_second):
    rows, cols, chans = latents.shape
    own = rows * cols
    flat = lambda w: jnp.transpose(w, (1, 2, 0, 3)).reshape(9, chans, chans)
    row = lambda v: v.reshape(1, chans)
    hbm = pl.BlockSpec(memory_space=pl.ANY)
    n_stat = 2 * chans // LANES
    out = pl.pallas_call(
        functools.partial(kernel, n_view, rows, cols, chans),
        out_shape=pltpu.VMEM((rows, 2, 2 * cols, chans), BF16),
        in_specs=[hbm] * 7,
        out_specs=pl.BlockSpec(memory_space=pltpu.VMEM),
        scratch_shapes=[
            pltpu.VMEM((rows + 4, cols, chans), BF16),
            pltpu.VMEM((4, 1, chans), F32),
            pltpu.VMEM((9, chans, chans), BF16),
            pltpu.VMEM((4, 3, chans, chans), BF16),
            pltpu.VMEM((9, chans, chans), BF16),
            pltpu.VMEM((9, chans, chans), BF16),
            pltpu.VMEM((3, rows + 4, cols, chans), BF16),
            pltpu.VMEM((4, 3, (rows // 2 + 1) * cols, chans), BF16),
            pltpu.VMEM((4, (rows // 2 + 1) * cols, chans), F32),
            pltpu.VMEM((3, own + 2 * cols, chans), BF16),
            pltpu.VMEM((3, own + cols, chans), BF16),
            pltpu.VMEM((chans // TILE, 2, own, TILE), F32),
            pltpu.VMEM((TILE // LANES, own * 4, LANES), F32),
            pltpu.VMEM((2 * rows + 6, chans // LANES, cols + 16, LANES), F32),
            pltpu.VMEM((n_stat, LANES), F32),
            pltpu.VMEM((n_view - 1, n_stat, LANES), F32),
            pltpu.SemaphoreType.DMA((rows,)),
            pltpu.SemaphoreType.DMA,
            pltpu.SemaphoreType.DMA((2,)),
            pltpu.SemaphoreType.DMA,
            pltpu.SemaphoreType.DMA((2,)),
            pltpu.SemaphoreType.DMA((2,)),
            pltpu.SemaphoreType.DMA,
            pltpu.SemaphoreType.DMA,
        ],
        compiler_params=pltpu.CompilerParams(
            collective_id=0, has_side_effects=True, vmem_limit_bytes=60 * 1024 * 1024
        ),
    )(
        latents, row(norm_gain), row(norm_shift), flat(w_first), row(bias_first), flat(w_second),
        row(bias_second),
    )
    return out.reshape(2 * rows, 2 * cols, chans)


def solution(mesh):
    placed = (P(("scene", "view"), None, None), P(), P(), P(), P(), P(), P())
    return jax.shard_map(
        functools.partial(per_device, mesh.shape["view"]),
        mesh=mesh,
        in_specs=placed,
        out_specs=P(("scene", "view"), None, None),
        check_vma=False,
    )
```

```python
import functools

import jax
import jax.numpy as jnp
from jax import lax
from jax.experimental import pallas as pl
from jax.experimental.pallas import tpu as pltpu
from jax.sharding import PartitionSpec as P

GROUPS = 32
H_LAT = 32
EPSILON = 1e-06
LANES = 128
TILE = 256
F32 = jnp.float32
BF16 = jnp.bfloat16


def dot_nt(x, w):
    return lax.dot_general(x, w, (((1,), (1,)), ((), ())), preferred_element_type=F32)


def dot_nn(x, w):
    return lax.dot_general(x, w, (((1,), (0,)), ((), ())), preferred_element_type=F32)


def kernel(
    n_view, rows, cols, chans,
    lat_hbm, gain_hbm, shift_hbm, w1_hbm, b1_hbm, w2_hbm, b2_hbm,
    out_ref,
    lat, small, w1, gt, w2, fold, act, vbuf, mbuf, mx, lhs_u, part, wide, edge, stat, stat_in,
    lat_sem, small_sem, w1_sem, w2_sem, halo_send, halo_recv, stat_send, stat_recv, ready, paired,
):
    me = lax.axis_index("view")
    slabs = H_LAT // rows
    assert slabs == 4
    views = n_view // slabs
    slab = me // views
    own = rows * cols
    has_up = slab > 0
    has_down = slab < slabs - 1

    barrier = pltpu.get_barrier_semaphore()

    hub = n_view - 2
    above, below = me - views, me + views
    first, second, third, last = slab == 0, slab == 1, slab == 2, slab == 3
    between = jnp.logical_or(second, third)
    rest = n_view - views
    unrolled = n_view <= 16

    def signal(to, carry=0):
        @pl.when(to != me)
        def _():
            pl.semaphore_signal(barrier, inc=1, device_id={"view": to})
        return carry

    def greet():
        lax.fori_loop(rest, n_view, signal, 0, unroll=unrolled)

        @pl.when(second)
        def _():
            signal(above)
            signal(below)

        @pl.when(first)
        def _():
            lax.fori_loop(views, rest, signal, 0, unroll=unrolled)

    def spread_word():
        @pl.when(me == hub)
        def _():
            pl.semaphore_wait(barrier, n_view - 1)

            def tell(to, carry):
                pl.semaphore_signal(ready, inc=1, device_id={"view": to})
                return carry

            lax.fori_loop(0, rest, tell, 0, unroll=unrolled)

    lat_rows = 1

    def lat_copy(i):
        some = pl.ds(i * lat_rows, lat_rows)
        return pltpu.make_async_copy(lat_hbm.at[some], lat.at[pl.ds(2 + i * lat_rows, lat_rows)], lat_sem.at[i])

    def small_copy(i):
        ref = (gain_hbm, shift_hbm, b1_hbm, b2_hbm)[i]
        return pltpu.make_async_copy(ref, small.at[i], small_sem)

    def w1_copy(t):
        return pltpu.make_async_copy(w1_hbm.at[t], w1.at[t], w1_sem.at[t // 5])

    def w2_copy(t):
        return pltpu.make_async_copy(w2_hbm.at[t], w2.at[t], w2_sem)

    for i in range(rows):
        lat_copy(i).start()
    greet()
    spread_word()
    for t in range(9):
        w1_copy(t).start(priority=1)
    for i in range(4):
        small_copy(i).start(priority=1)

    tiles = chans // TILE
    eye = (
        lax.broadcasted_iota(jnp.int32, (TILE, TILE), 0) == lax.broadcasted_iota(jnp.int32, (TILE, TILE), 1)
    ).astype(F32).astype(BF16)

    def prepare(j, carry):
        k0 = pl.multiple_of(j // tiles * TILE, TILE)
        n0 = pl.multiple_of(lax.rem(j, tiles) * TILE, TILE)
        for s in range(3):
            for k, r in ((0, 0), (3, 2)):
                g = w1[3 * r + s, pl.ds(n0, TILE), pl.ds(k0, TILE)]
                gt[k, s, pl.ds(k0, TILE), pl.ds(n0, TILE)] = dot_nt(eye, g).astype(BF16)
            for a in range(0, TILE, LANES):
                for b in range(0, TILE, LANES):
                    n_at, k_at = pl.ds(n0 + a, LANES), pl.ds(k0 + b, LANES)
                    h = [w1[3 * r + s, n_at, k_at].astype(F32) for r in range(3)]
                    even = (h[0] + h[2]) * 0.5
                    odd = h[1] * 0.5
                    gt[1, s, k_at, n_at] = (even + odd).astype(BF16).T
                    gt[2, s, k_at, n_at] = (even - odd).astype(BF16).T
        return carry

    def prepare_all():
        pltpu.make_async_copy(w1.at[pl.ds(0, 5)], w1.at[pl.ds(0, 5)], w1_sem.at[0]).wait()
        for t in range(9):
            w2_copy(t).start(priority=1)
        pltpu.make_async_copy(w1.at[pl.ds(5, 4)], w1.at[pl.ds(5, 4)], w1_sem.at[1]).wait()
        lax.fori_loop(0, tiles * tiles, prepare, 0)

    sums = jnp.zeros((8, chans), F32)
    squares = jnp.zeros((8, chans), F32)
    for i in range(rows):
        if i % lat_rows == 0:
            lat_copy(i // lat_rows).wait()
        x = lat[2 + i].astype(F32).reshape(cols // 8, 8, chans)
        sums = sums + jnp.sum(x, axis=0)
        squares = squares + jnp.sum(x * x, axis=0)
    sums = jnp.sum(sums, axis=0, keepdims=True)
    squares = jnp.sum(squares, axis=0, keepdims=True)
    blocks = chans // LANES
    stat[...] = jnp.concatenate(
        [v[:, k * LANES : (k + 1) * LANES] for v in (sums, squares) for k in range(blocks)], axis=0
    )

    up_copy = pltpu.make_async_remote_copy(
        src_ref=lat.at[pl.ds(2, 2)], dst_ref=lat.at[pl.ds(rows + 2, 2)],
        send_sem=halo_send.at[0], recv_sem=halo_recv.at[0],
        device_id={"view": jnp.maximum(above, 0)},
    )
    down_copy = pltpu.make_async_remote_copy(
        src_ref=lat.at[pl.ds(rows, 2)], dst_ref=lat.at[pl.ds(0, 2)],
        send_sem=halo_send.at[1], recv_sem=halo_recv.at[1],
        device_id={"view": jnp.minimum(below, n_view - 1)},
    )
    own_up = pltpu.make_async_copy(lat_hbm.at[pl.ds(0, 2)], lat.at[pl.ds(0, 2)], halo_recv.at[1])
    own_down = pltpu.make_async_copy(lat_hbm.at[pl.ds(0, 2)], lat.at[pl.ds(rows + 2, 2)], halo_recv.at[0])

    def send_halos(*pairs):
        for when, copy in pairs:
            @pl.when(when)
            def _():
                copy.start()

    def send_stat(to, carry):
        @pl.when(to != me)
        def _():
            slot = lax.rem(to - me + n_view, n_view) - 1
            pltpu.make_async_remote_copy(
                src_ref=stat, dst_ref=stat_in.at[slot], send_sem=stat_send, recv_sem=stat_recv,
                device_id={"view": to},
            ).start()
        return carry

    @pl.when(first)
    def _():
        pl.semaphore_wait(barrier, 1)

    @pl.when(third)
    def _():
        pl.semaphore_wait(barrier, views + 1)
        pl.semaphore_signal(paired, inc=1, device_id={"view": above})

    @pl.when(second)
    def _():
        pl.semaphore_wait(barrier, views)

    @pl.when(between)
    def _():
        lax.fori_loop(0, views, send_stat, 0, unroll=unrolled)

    send_halos((first, own_up), (first, down_copy), (between, up_copy))

    @pl.when(second)
    def _():
        pl.semaphore_wait(paired, 1)

    send_halos((second, down_copy))

    @pl.when(first)
    def _():
        prepare_all()

    @pl.when(jnp.logical_not(last))
    def _():
        pl.semaphore_wait(ready, 1)

    @pl.when(jnp.logical_and(last, me != hub))
    def _():
        pl.semaphore_wait(barrier, n_view - 1)

    @pl.when(jnp.logical_not(between))
    def _():
        lax.fori_loop(0, views, send_stat, 0, unroll=unrolled)

    lax.fori_loop(views, n_view, send_stat, 0, unroll=unrolled)
    send_halos(
        (last, up_copy), (third, down_copy), (last, own_down)
    )

    @pl.when(has_up)
    def _():
        prepare_all()

    zeros = jnp.zeros((edge.shape[1], 8, LANES), F32)

    def clear(k, carry):
        edge[k, :, pl.ds(0, 8)] = zeros
        edge[k, :, pl.ds(cols + 8, 8)] = zeros
        return carry

    lax.fori_loop(0, edge.shape[0], clear, 0)
    pltpu.make_async_copy(w2, w2, w2_sem).wait()

    def fold_tile(j, carry):
        k0 = pl.multiple_of(j // tiles * TILE, TILE)
        n0 = pl.multiple_of(lax.rem(j, tiles) * TILE, TILE)
        for k, t in enumerate((0, 2, 6, 8)):
            g = w2[t, pl.ds(n0, TILE), pl.ds(k0, TILE)]
            fold[5 + k, pl.ds(k0, TILE), pl.ds(n0, TILE)] = dot_nt(eye, g).astype(BF16)
        for a in range(0, TILE, LANES):
            for b in range(0, TILE, LANES):
                n_at, k_at = pl.ds(n0 + a, LANES), pl.ds(k0 + b, LANES)

                def add(*taps):
                    terms = [w2[t, n_at, k_at].astype(F32) for t in taps]
                    return terms[0] + terms[1] + terms[2]

                def put(i, v):
                    fold[i, k_at, n_at] = v.astype(BF16).T

                put(3, add(0, 1, 2))
                put(4, add(6, 7, 8))
                left = add(0, 3, 6)
                put(1, left)
                right = add(2, 5, 8)
                put(2, right)
                put(0, left + add(1, 4, 7) + right)
        return carry

    lax.fori_loop(0, tiles * tiles, fold_tile, 0)
    pltpu.make_async_copy(small, small, small_sem).wait()

    same = (
        lax.broadcasted_iota(jnp.int32, (LANES, LANES), 0) // (chans // GROUPS)
        == lax.broadcasted_iota(jnp.int32, (LANES, LANES), 1) // (chans // GROUPS)
    ).astype(F32).astype(BF16)

    pltpu.make_async_copy(stat_in, stat_in, stat_recv).wait()

    total = stat[...] + jnp.sum(stat_in[...], axis=0)
    high = total.astype(BF16).astype(F32)
    rest = total - high
    middle = rest.astype(BF16).astype(F32)
    low = rest - middle
    parts = jnp.concatenate([high, middle, low, jnp.zeros_like(low)], axis=0).astype(BF16)
    sized = dot_nn(parts, same)
    n_stat = 2 * blocks
    total = sized[:n_stat] + sized[n_stat : 2 * n_stat] + sized[2 * n_stat : 3 * n_stat]
    entries = float(own * (chans // GROUPS) * n_view)
    mean = total[:blocks] / entries
    var = total[blocks:] / entries - mean * mean
    inv = lax.rsqrt(var + EPSILON)

    def one_row(v):
        return jnp.concatenate([v[k : k + 1] for k in range(blocks)], axis=1)

    scale = one_row(inv) * small[0]
    offset = small[1] - one_row(mean) * scale
    half_scale = scale * 0.5
    half_offset = offset * 0.5

    groups = range(chans // LANES)

    def beside(slot, g, x):
        edge[slot, g, pl.ds(8, cols)] = x
        return edge[slot, g, pl.ds(7, cols)], edge[slot, g, pl.ds(9, cols)]

    def activate(i):
        for g in groups:
            lanes = pl.ds(g * LANES, LANES)
            side = slice(g * LANES, (g + 1) * LANES)
            h = lat[i, :, lanes].astype(F32) * half_scale[:, side] + half_offset[:, side]
            a = h + h * jnp.tanh(h)
            if i < 2:
                a = jnp.where(has_up, a, 0.0)
            if i >= rows + 2:
                a = jnp.where(has_down, a, 0.0)
            left, right = beside(i, g, a)
            act[0, i, :, lanes] = left.astype(BF16)
            act[1, i, :, lanes] = a.astype(BF16)
            act[2, i, :, lanes] = right.astype(BF16)

    pairs = list(range(rows // 2 + 1))
    place = {p: p for p in pairs}

    def arrange(k, pairs):
        a, b = ((0, 2), (1, 2), (2, 1), (1, 3))[k]
        for p in pairs:
            at = pl.ds(place[p] * cols, cols)
            for s in range(3):
                x, y = act[s, 2 * p + a], act[s, 2 * p + b]
                vbuf[k, s, at] = x + y if k == 1 else x - y

    def products(n, k, pairs):
        at = pl.ds(place[pairs[0]] * cols, len(pairs) * cols)
        lanes = pl.ds(n * TILE, TILE)
        terms = [dot_nn(vbuf[k, s, at], gt[k, s, :, lanes]) for s in range(3)]
        mbuf[k, at, lanes] = terms[0] + terms[1] + terms[2]

    bias1 = small[2]

    def mix(n, i):
        p, odd = i // 2, i % 2
        at = pl.ds(place[p] * cols, cols)
        for g in groups[n * TILE // LANES : (n + 1) * TILE // LANES]:
            lanes = pl.ds(g * LANES, LANES)
            v = [mbuf[k, at, lanes] for k in ((1, 2, 3) if odd else (0, 1, 2))]
            conv = v[0] - v[1] - v[2] if odd else v[0] + v[1] + v[2]
            m = lat[i + 1, :, lanes].astype(F32) + conv + bias1[:, g * LANES : (g + 1) * LANES]
            if i == 0:
                m = jnp.where(has_up, m, 0.0)
            if i == rows + 1:
                m = jnp.where(has_down, m, 0.0)
            narrow = m.astype(BF16)
            m = narrow.astype(F32)
            to = pl.ds(i * cols, cols)
            left, right = beside(rows + 4 + i, g, m)
            mx[0, to, lanes] = narrow
            mx[1, to, lanes] = left.astype(BF16) - narrow
            mx[2, to, lanes] = right.astype(BF16) - narrow

    def rise_of(n, j):
        lanes = pl.ds(n * TILE, TILE)
        here, below = pl.ds(j * cols, cols), pl.ds((j + 1) * cols, cols)
        for s in range(3):
            lhs_u[s, here, lanes] = mx[s, below, lanes] - mx[s, here, lanes]

    width = TILE
    bias2 = small[3]

    def take(ref, s, pieces):
        return jnp.concatenate([ref[s, pl.ds(a * cols, b * cols)] for a, b in pieces], axis=0)

    def level(n, pieces):
        lanes = pl.ds(n * width, width)
        mine = [(a + 1, b) for a, b in pieces]
        base = dot_nn(take(mx, 0, mine), fold[0, :, lanes]) + bias2[:, n * width : (n + 1) * width]
        for q in range(2):
            both = base + dot_nn(take(mx, 1 + q, mine), fold[1 + q, :, lanes])
            done = 0
            for a, b in pieces:
                part[n, q, pl.ds(a * cols, b * cols)] = both[done * cols : (done + b) * cols]
                done += b

    def finish(n, p, pieces):
        lanes = pl.ds(n * width, width)
        mine = [(a + p, b) for a, b in pieces]
        rise = dot_nn(take(lhs_u, 0, mine), fold[3 + p, :, lanes])
        for q in range(2):
            term = rise + dot_nn(take(lhs_u, 1 + q, mine), fold[5 + 2 * p + q, :, lanes])
            done = 0
            for a, b in pieces:
                for i in range(a, a + b):
                    for g in range(width // LANES):
                        x = part[n, q, pl.ds(i * cols, cols), pl.ds(g * LANES, LANES)]
                        y = term[done * cols : (done + 1) * cols, g * LANES : (g + 1) * LANES]
                        wide[g, pl.ds((p * rows + i) * 2 * cols + q, cols, 2), :] = x + y if p else x - y
                    done += 1
        for a, b in pieces:
            for i in range(a, a + b):
                for g in range(width // LANES):
                    tile = wide[g, pl.ds((p * rows + i) * 2 * cols, 2 * cols), :].astype(BF16)
                    out_ref[i, p, :, pl.ds(n * width + g * LANES, LANES)] = tile

    columns = range(chans // width)

    for i in range(2, rows + 2, 2):
        activate(i)

    own_up.wait()
    own_down.wait()
    for i in (0, rows + 2):
        activate(i)
    arrange(0, pairs)
    for n in columns:
        products(n, 0, pairs)
    for i in range(1, rows + 4, 2):
        activate(i)
    for n in columns:
        for k in range(1, 4):
            if n == 0:
                arrange(k, pairs)
            products(n, k, pairs)
        if n:
            for i in range(rows + 2):
                mix(n - 1, i)
    for i in range(rows + 2):
        mix(columns[-1], i)
    for n in columns:
        level(n, [(0, rows)])
    for n in columns:
        for j in range(rows + 1):
            rise_of(n, j)
    for n in columns:
        for p in range(2):
            finish(n, p, [(0, rows)])

    pltpu.make_async_copy(stat_in, stat_in, stat_send).wait()

    @pl.when(has_up)
    def _():
        up_copy.wait_send()

    @pl.when(has_down)
    def _():
        down_copy.wait_send()


def per_device(n_view, latents, norm_gain, norm_shift, w_first, bias_first, w_second, bias_second):
    rows, cols, chans = latents.shape
    own = rows * cols
    flat = lambda w: jnp.transpose(w, (1, 2, 0, 3)).reshape(9, chans, chans)
    row = lambda v: v.reshape(1, chans)
    hbm = pl.BlockSpec(memory_space=pl.ANY)
    n_stat = 2 * chans // LANES
    out = pl.pallas_call(
        functools.partial(kernel, n_view, rows, cols, chans),
        out_shape=pltpu.VMEM((rows, 2, 2 * cols, chans), BF16),
        in_specs=[hbm] * 7,
        out_specs=pl.BlockSpec(memory_space=pltpu.VMEM),
        scratch_shapes=[
            pltpu.VMEM((rows + 4, cols, chans), BF16),
            pltpu.VMEM((4, 1, chans), F32),
            pltpu.VMEM((9, chans, chans), BF16),
            pltpu.VMEM((4, 3, chans, chans), BF16),
            pltpu.VMEM((9, chans, chans), BF16),
            pltpu.VMEM((9, chans, chans), BF16),
            pltpu.VMEM((3, rows + 4, cols, chans), BF16),
            pltpu.VMEM((4, 3, (rows // 2 + 1) * cols, chans), BF16),
            pltpu.VMEM((4, (rows // 2 + 1) * cols, chans), F32),
            pltpu.VMEM((3, own + 2 * cols, chans), BF16),
            pltpu.VMEM((3, own + cols, chans), BF16),
            pltpu.VMEM((chans // TILE, 2, own, TILE), F32),
            pltpu.VMEM((TILE // LANES, own * 4, LANES), F32),
            pltpu.VMEM((2 * rows + 6, chans // LANES, cols + 16, LANES), F32),
            pltpu.VMEM((n_stat, LANES), F32),
            pltpu.VMEM((n_view - 1, n_stat, LANES), F32),
            pltpu.SemaphoreType.DMA((rows,)),
            pltpu.SemaphoreType.DMA,
            pltpu.SemaphoreType.DMA((2,)),
            pltpu.SemaphoreType.DMA,
            pltpu.SemaphoreType.DMA((2,)),
            pltpu.SemaphoreType.DMA((2,)),
            pltpu.SemaphoreType.DMA,
            pltpu.SemaphoreType.DMA,
            pltpu.SemaphoreType.REGULAR,
            pltpu.SemaphoreType.REGULAR,
        ],
        compiler_params=pltpu.CompilerParams(
            collective_id=0, has_side_effects=True, vmem_limit_bytes=60 * 1024 * 1024
        ),
    )(
        latents, row(norm_gain), row(norm_shift), flat(w_first), row(bias_first), flat(w_second),
        row(bias_second),
    )
    return out.reshape(2 * rows, 2 * cols, chans)


def solution(mesh):
    placed = (P(("scene", "view"), None, None), P(), P(), P(), P(), P(), P())
    return jax.shard_map(
        functools.partial(per_device, mesh.shape["view"]),
        mesh=mesh,
        in_specs=placed,
        out_specs=P(("scene", "view"), None, None),
        check_vma=False,
    )
```

```python
import functools

import jax
import jax.numpy as jnp
from jax import lax
from jax.experimental import pallas as pl
from jax.experimental.pallas import tpu as pltpu
from jax.sharding import PartitionSpec as P

GROUPS = 32
H_LAT = 32
EPSILON = 1e-06
LANES = 128
TILE = 256
F32 = jnp.float32
BF16 = jnp.bfloat16


def dot_nt(x, w):
    return lax.dot_general(x, w, (((1,), (1,)), ((), ())), preferred_element_type=F32)


def dot_nn(x, w):
    return lax.dot_general(x, w, (((1,), (0,)), ((), ())), preferred_element_type=F32)


def kernel(
    n_view, rows, cols, chans,
    lat_hbm, gain_hbm, shift_hbm, w1_hbm, b1_hbm, w2_hbm, b2_hbm,
    out_ref,
    lat, small, w1, gt, w2, fold, act, vbuf, mbuf, mx, lhs_u, part, wide, edge, raised, stat, stat_in,
    lat_sem, small_sem, w1_sem, w2_sem, halo_send, halo_recv, stat_send, stat_recv, ready, paired,
):
    me = lax.axis_index("view")
    slabs = H_LAT // rows
    assert slabs == 4
    views = n_view // slabs
    slab = me // views
    own = rows * cols
    has_up = slab > 0
    has_down = slab < slabs - 1

    barrier = pltpu.get_barrier_semaphore()

    hub = n_view - 2
    above, below = me - views, me + views
    first, second, third, last = slab == 0, slab == 1, slab == 2, slab == 3
    between = jnp.logical_or(second, third)
    rest = n_view - views
    unrolled = n_view <= 16

    def signal(to, carry=0):
        @pl.when(to != me)
        def _():
            pl.semaphore_signal(barrier, inc=1, device_id={"view": to})
        return carry

    def greet():
        lax.fori_loop(rest, n_view, signal, 0, unroll=unrolled)

        @pl.when(second)
        def _():
            signal(above)
            signal(below)

        @pl.when(first)
        def _():
            lax.fori_loop(views, rest, signal, 0, unroll=unrolled)

    def spread_word():
        @pl.when(me == hub)
        def _():
            pl.semaphore_wait(barrier, n_view - 1)

            def tell(to, carry):
                pl.semaphore_signal(ready, inc=1, device_id={"view": to})
                return carry

            lax.fori_loop(0, rest, tell, 0, unroll=unrolled)

    lat_rows = 1

    def lat_copy(i):
        some = pl.ds(i * lat_rows, lat_rows)
        return pltpu.make_async_copy(lat_hbm.at[some], lat.at[pl.ds(2 + i * lat_rows, lat_rows)], lat_sem.at[i])

    def small_copy(i):
        ref = (gain_hbm, shift_hbm, b1_hbm, b2_hbm)[i]
        return pltpu.make_async_copy(ref, small.at[i], small_sem)

    def w1_copy(t):
        return pltpu.make_async_copy(w1_hbm.at[t], w1.at[t], w1_sem.at[t // 5])

    def w2_copy(t):
        return pltpu.make_async_copy(w2_hbm.at[t], w2.at[t], w2_sem)

    for i in range(rows):
        lat_copy(i).start()
    greet()
    spread_word()
    for t in range(9):
        w1_copy(t).start(priority=1)
    for i in range(4):
        small_copy(i).start(priority=1)

    tiles = chans // TILE
    eye = (
        lax.broadcasted_iota(jnp.int32, (TILE, TILE), 0) == lax.broadcasted_iota(jnp.int32, (TILE, TILE), 1)
    ).astype(F32).astype(BF16)

    def prepare(j, carry):
        k0 = pl.multiple_of(j // tiles * TILE, TILE)
        n0 = pl.multiple_of(lax.rem(j, tiles) * TILE, TILE)
        for s in range(3):
            for k, r in ((0, 0), (3, 2)):
                g = w1[3 * r + s, pl.ds(n0, TILE), pl.ds(k0, TILE)]
                gt[k, s, pl.ds(k0, TILE), pl.ds(n0, TILE)] = dot_nt(eye, g).astype(BF16)
            for a in range(0, TILE, LANES):
                for b in range(0, TILE, LANES):
                    n_at, k_at = pl.ds(n0 + a, LANES), pl.ds(k0 + b, LANES)
                    h = [w1[3 * r + s, n_at, k_at].astype(F32) for r in range(3)]
                    even = (h[0] + h[2]) * 0.5
                    odd = h[1] * 0.5
                    gt[1, s, k_at, n_at] = (even + odd).astype(BF16).T
                    gt[2, s, k_at, n_at] = (even - odd).astype(BF16).T
        return carry

    def prepare_all():
        pltpu.make_async_copy(w1.at[pl.ds(0, 5)], w1.at[pl.ds(0, 5)], w1_sem.at[0]).wait()
        for t in range(9):
            w2_copy(t).start(priority=1)
        pltpu.make_async_copy(w1.at[pl.ds(5, 4)], w1.at[pl.ds(5, 4)], w1_sem.at[1]).wait()
        lax.fori_loop(0, tiles * tiles, prepare, 0)

    sums = jnp.zeros((8, chans), F32)
    squares = jnp.zeros((8, chans), F32)
    for i in range(rows):
        if i % lat_rows == 0:
            lat_copy(i // lat_rows).wait()
        x = lat[2 + i].astype(F32).reshape(cols // 8, 8, chans)
        sums = sums + jnp.sum(x, axis=0)
        squares = squares + jnp.sum(x * x, axis=0)
    sums = jnp.sum(sums, axis=0, keepdims=True)
    squares = jnp.sum(squares, axis=0, keepdims=True)
    blocks = chans // LANES
    stat[...] = jnp.concatenate(
        [v[:, k * LANES : (k + 1) * LANES] for v in (sums, squares) for k in range(blocks)], axis=0
    )

    up_copy = pltpu.make_async_remote_copy(
        src_ref=lat.at[pl.ds(2, 2)], dst_ref=lat.at[pl.ds(rows + 2, 2)],
        send_sem=halo_send.at[0], recv_sem=halo_recv.at[0],
        device_id={"view": jnp.maximum(above, 0)},
    )
    down_copy = pltpu.make_async_remote_copy(
        src_ref=lat.at[pl.ds(rows, 2)], dst_ref=lat.at[pl.ds(0, 2)],
        send_sem=halo_send.at[1], recv_sem=halo_recv.at[1],
        device_id={"view": jnp.minimum(below, n_view - 1)},
    )
    own_up = pltpu.make_async_copy(lat_hbm.at[pl.ds(0, 2)], lat.at[pl.ds(0, 2)], halo_recv.at[1])
    own_down = pltpu.make_async_copy(lat_hbm.at[pl.ds(0, 2)], lat.at[pl.ds(rows + 2, 2)], halo_recv.at[0])

    def send_halos(*pairs):
        for when, copy in pairs:
            @pl.when(when)
            def _():
                copy.start()

    def send_stat(to, carry):
        @pl.when(to != me)
        def _():
            slot = lax.rem(to - me + n_view, n_view) - 1
            pltpu.make_async_remote_copy(
                src_ref=stat, dst_ref=stat_in.at[slot], send_sem=stat_send, recv_sem=stat_recv,
                device_id={"view": to},
            ).start()
        return carry

    @pl.when(first)
    def _():
        pl.semaphore_wait(barrier, 1)

    @pl.when(third)
    def _():
        pl.semaphore_wait(barrier, views + 1)
        pl.semaphore_signal(paired, inc=1, device_id={"view": above})

    @pl.when(second)
    def _():
        pl.semaphore_wait(barrier, views)

    @pl.when(between)
    def _():
        lax.fori_loop(0, views, send_stat, 0, unroll=unrolled)

    send_halos((first, own_up), (first, down_copy), (between, up_copy))

    @pl.when(second)
    def _():
        pl.semaphore_wait(paired, 1)

    send_halos((second, down_copy))

    @pl.when(first)
    def _():
        prepare_all()

    @pl.when(jnp.logical_not(last))
    def _():
        pl.semaphore_wait(ready, 1)

    @pl.when(jnp.logical_and(last, me != hub))
    def _():
        pl.semaphore_wait(barrier, n_view - 1)

    @pl.when(jnp.logical_not(between))
    def _():
        lax.fori_loop(0, views, send_stat, 0, unroll=unrolled)

    lax.fori_loop(views, n_view, send_stat, 0, unroll=unrolled)
    send_halos(
        (last, up_copy), (third, down_copy), (last, own_down)
    )

    @pl.when(has_up)
    def _():
        prepare_all()

    zeros = jnp.zeros((edge.shape[1], 8, LANES), F32)

    def clear(k, carry):
        edge[k, :, pl.ds(0, 8)] = zeros
        edge[k, :, pl.ds(cols + 8, 8)] = zeros
        return carry

    lax.fori_loop(0, edge.shape[0], clear, 0)
    pltpu.make_async_copy(w2, w2, w2_sem).wait()

    def fold_tile(j, carry):
        k0 = pl.multiple_of(j // tiles * TILE, TILE)
        n0 = pl.multiple_of(lax.rem(j, tiles) * TILE, TILE)
        for k, t in enumerate((0, 2, 6, 8)):
            g = w2[t, pl.ds(n0, TILE), pl.ds(k0, TILE)]
            fold[5 + k, pl.ds(k0, TILE), pl.ds(n0, TILE)] = dot_nt(eye, g).astype(BF16)
        for a in range(0, TILE, LANES):
            for b in range(0, TILE, LANES):
                n_at, k_at = pl.ds(n0 + a, LANES), pl.ds(k0 + b, LANES)

                def add(*taps):
                    terms = [w2[t, n_at, k_at].astype(F32) for t in taps]
                    return terms[0] + terms[1] + terms[2]

                def put(i, v):
                    fold[i, k_at, n_at] = v.astype(BF16).T

                put(3, add(0, 1, 2))
                put(4, add(6, 7, 8))
                left = add(0, 3, 6)
                put(1, left)
                right = add(2, 5, 8)
                put(2, right)
                put(0, left + add(1, 4, 7) + right)
        return carry

    lax.fori_loop(0, tiles * tiles, fold_tile, 0)
    pltpu.make_async_copy(small, small, small_sem).wait()

    def raise_row(i, carry):
        raised[i] = lat[2 + i].astype(F32) + small[2]
        return carry

    lax.fori_loop(0, rows, raise_row, 0)

    same = (
        lax.broadcasted_iota(jnp.int32, (LANES, LANES), 0) // (chans // GROUPS)
        == lax.broadcasted_iota(jnp.int32, (LANES, LANES), 1) // (chans // GROUPS)
    ).astype(F32).astype(BF16)

    pltpu.make_async_copy(stat_in, stat_in, stat_recv).wait()

    total = stat[...] + jnp.sum(stat_in[...], axis=0)
    high = total.astype(BF16).astype(F32)
    rest = total - high
    middle = rest.astype(BF16).astype(F32)
    low = rest - middle
    parts = jnp.concatenate([high, middle, low, jnp.zeros_like(low)], axis=0).astype(BF16)
    sized = dot_nn(parts, same)
    n_stat = 2 * blocks
    total = sized[:n_stat] + sized[n_stat : 2 * n_stat] + sized[2 * n_stat : 3 * n_stat]
    entries = float(own * (chans // GROUPS) * n_view)
    mean = total[:blocks] * (1.0 / entries)
    var = total[blocks:] * (1.0 / entries) - mean * mean
    inv = lax.rsqrt(var + EPSILON)

    def one_row(v):
        return jnp.concatenate([v[k : k + 1] for k in range(blocks)], axis=1)

    scale = one_row(inv) * small[0]
    offset = small[1] - one_row(mean) * scale
    half_scale = scale * 0.5
    half_offset = offset * 0.5

    groups = range(chans // LANES)

    def beside(slot, g, x):
        edge[slot, g, pl.ds(8, cols)] = x
        return edge[slot, g, pl.ds(7, cols)], edge[slot, g, pl.ds(9, cols)]

    def activate(i):
        for g in groups:
            lanes = pl.ds(g * LANES, LANES)
            side = slice(g * LANES, (g + 1) * LANES)
            h = lat[i, :, lanes].astype(F32) * half_scale[:, side] + half_offset[:, side]
            a = h + h * jnp.tanh(h)
            if i < 2:
                a = jnp.where(has_up, a, 0.0)
            if i >= rows + 2:
                a = jnp.where(has_down, a, 0.0)
            left, right = beside(i, g, a)
            act[0, i, :, lanes] = left.astype(BF16)
            act[1, i, :, lanes] = a.astype(BF16)
            act[2, i, :, lanes] = right.astype(BF16)

    pairs = list(range(rows // 2 + 1))
    place = {p: p for p in pairs}

    def arrange(k, pairs):
        a, b = ((0, 2), (1, 2), (2, 1), (1, 3))[k]
        for p in pairs:
            at = pl.ds(place[p] * cols, cols)
            for s in range(3):
                x, y = act[s, 2 * p + a], act[s, 2 * p + b]
                vbuf[k, s, at] = x + y if k == 1 else x - y

    def products(n, k, pairs):
        at = pl.ds(place[pairs[0]] * cols, len(pairs) * cols)
        lanes = pl.ds(n * TILE, TILE)
        terms = [dot_nn(vbuf[k, s, at], gt[k, s, :, lanes]) for s in range(3)]
        mbuf[k, at, lanes] = terms[0] + terms[1] + terms[2]

    bias1 = small[2]

    def mix(n, i):
        p, odd = i // 2, i % 2
        at = pl.ds(place[p] * cols, cols)
        for g in groups[n * TILE // LANES : (n + 1) * TILE // LANES]:
            lanes = pl.ds(g * LANES, LANES)
            v = [mbuf[k, at, lanes] for k in ((1, 2, 3) if odd else (0, 1, 2))]
            conv = v[0] - v[1] - v[2] if odd else v[0] + v[1] + v[2]
            if 1 <= i <= rows:
                m = raised[i - 1, :, lanes] + conv
            else:
                m = lat[i + 1, :, lanes].astype(F32) + conv + bias1[:, g * LANES : (g + 1) * LANES]
            if i == 0:
                m = jnp.where(has_up, m, 0.0)
            if i == rows + 1:
                m = jnp.where(has_down, m, 0.0)
            narrow = m.astype(BF16)
            m = narrow.astype(F32)
            to = pl.ds(i * cols, cols)
            left, right = beside(rows + 4 + i, g, m)
            mx[0, to, lanes] = narrow
            mx[1, to, lanes] = left.astype(BF16) - narrow
            mx[2, to, lanes] = right.astype(BF16) - narrow

    def rise_of(n, j):
        lanes = pl.ds(n * TILE, TILE)
        here, below = pl.ds(j * cols, cols), pl.ds((j + 1) * cols, cols)
        for s in range(3):
            lhs_u[s, here, lanes] = mx[s, below, lanes] - mx[s, here, lanes]

    width = TILE
    bias2 = small[3]

    def take(ref, s, pieces):
        return jnp.concatenate([ref[s, pl.ds(a * cols, b * cols)] for a, b in pieces], axis=0)

    def level(n, pieces):
        lanes = pl.ds(n * width, width)
        mine = [(a + 1, b) for a, b in pieces]
        base = dot_nn(take(mx, 0, mine), fold[0, :, lanes]) + bias2[:, n * width : (n + 1) * width]
        for q in range(2):
            both = base + dot_nn(take(mx, 1 + q, mine), fold[1 + q, :, lanes])
            done = 0
            for a, b in pieces:
                part[n, q, pl.ds(a * cols, b * cols)] = both[done * cols : (done + b) * cols]
                done += b

    def finish(n, p, pieces):
        lanes = pl.ds(n * width, width)
        mine = [(a + p, b) for a, b in pieces]
        rise = dot_nn(take(lhs_u, 0, mine), fold[3 + p, :, lanes])
        for q in range(2):
            term = rise + dot_nn(take(lhs_u, 1 + q, mine), fold[5 + 2 * p + q, :, lanes])
            done = 0
            for a, b in pieces:
                for i in range(a, a + b):
                    for g in range(width // LANES):
                        x = part[n, q, pl.ds(i * cols, cols), pl.ds(g * LANES, LANES)]
                        y = term[done * cols : (done + 1) * cols, g * LANES : (g + 1) * LANES]
                        wide[g, pl.ds((p * rows + i) * 2 * cols + q, cols, 2), :] = x + y if p else x - y
                    done += 1
        for a, b in pieces:
            for i in range(a, a + b):
                for g in range(width // LANES):
                    tile = wide[g, pl.ds((p * rows + i) * 2 * cols, 2 * cols), :].astype(BF16)
                    out_ref[i, p, :, pl.ds(n * width + g * LANES, LANES)] = tile

    columns = range(chans // width)

    for i in range(2, rows + 2, 2):
        activate(i)

    own_up.wait()
    own_down.wait()
    for i in (0, rows + 2):
        activate(i)
    arrange(0, pairs)
    for n in columns:
        products(n, 0, pairs)
    for i in range(1, rows + 4, 2):
        activate(i)
    for n in columns:
        for k in (3, 1, 2):
            if n == 0:
                arrange(k, pairs)
            products(n, k, pairs)
        if n:
            for i in range(rows + 2):
                mix(n - 1, i)
    for i in range(rows + 2):
        mix(columns[-1], i)
    for n in columns:
        for j in range(rows + 1):
            rise_of(n, j)
    for n in columns:
        level(n, [(0, rows)])
        for p in range(2):
            finish(n, p, [(0, rows)])

    pltpu.make_async_copy(stat_in, stat_in, stat_send).wait()

    @pl.when(has_up)
    def _():
        up_copy.wait_send()

    @pl.when(has_down)
    def _():
        down_copy.wait_send()


def per_device(n_view, latents, norm_gain, norm_shift, w_first, bias_first, w_second, bias_second):
    rows, cols, chans = latents.shape
    own = rows * cols
    flat = lambda w: jnp.transpose(w, (1, 2, 0, 3)).reshape(9, chans, chans)
    row = lambda v: v.reshape(1, chans)
    hbm = pl.BlockSpec(memory_space=pl.ANY)
    n_stat = 2 * chans // LANES
    out = pl.pallas_call(
        functools.partial(kernel, n_view, rows, cols, chans),
        out_shape=pltpu.VMEM((rows, 2, 2 * cols, chans), BF16),
        in_specs=[hbm] * 7,
        out_specs=pl.BlockSpec(memory_space=pltpu.VMEM),
        scratch_shapes=[
            pltpu.VMEM((rows + 4, cols, chans), BF16),
            pltpu.VMEM((4, 1, chans), F32),
            pltpu.VMEM((9, chans, chans), BF16),
            pltpu.VMEM((4, 3, chans, chans), BF16),
            pltpu.VMEM((9, chans, chans), BF16),
            pltpu.VMEM((9, chans, chans), BF16),
            pltpu.VMEM((3, rows + 4, cols, chans), BF16),
            pltpu.VMEM((4, 3, (rows // 2 + 1) * cols, chans), BF16),
            pltpu.VMEM((4, (rows // 2 + 1) * cols, chans), F32),
            pltpu.VMEM((3, own + 2 * cols, chans), BF16),
            pltpu.VMEM((3, own + cols, chans), BF16),
            pltpu.VMEM((chans // TILE, 2, own, TILE), F32),
            pltpu.VMEM((TILE // LANES, own * 4, LANES), F32),
            pltpu.VMEM((2 * rows + 6, chans // LANES, cols + 16, LANES), F32),
            pltpu.VMEM((rows, cols, chans), F32),
            pltpu.VMEM((n_stat, LANES), F32),
            pltpu.VMEM((n_view - 1, n_stat, LANES), F32),
            pltpu.SemaphoreType.DMA((rows,)),
            pltpu.SemaphoreType.DMA,
            pltpu.SemaphoreType.DMA((2,)),
            pltpu.SemaphoreType.DMA,
            pltpu.SemaphoreType.DMA((2,)),
            pltpu.SemaphoreType.DMA((2,)),
            pltpu.SemaphoreType.DMA,
            pltpu.SemaphoreType.DMA,
            pltpu.SemaphoreType.REGULAR,
            pltpu.SemaphoreType.REGULAR,
        ],
        compiler_params=pltpu.CompilerParams(
            collective_id=0, has_side_effects=True, vmem_limit_bytes=60 * 1024 * 1024
        ),
    )(
        latents, row(norm_gain), row(norm_shift), flat(w_first), row(bias_first), flat(w_second),
        row(bias_second),
    )
    return out.reshape(2 * rows, 2 * cols, chans)


def solution(mesh):
    placed = (P(("scene", "view"), None, None), P(), P(), P(), P(), P(), P())
    return jax.shard_map(
        functools.partial(per_device, mesh.shape["view"]),
        mesh=mesh,
        in_specs=placed,
        out_specs=P(("scene", "view"), None, None),
        check_vma=False,
    )
```

```python
import functools

import jax
import jax.numpy as jnp
from jax import lax
from jax.experimental import pallas as pl
from jax.experimental.pallas import tpu as pltpu
from jax.sharding import PartitionSpec as P

GROUPS = 32
H_LAT = 32
EPSILON = 1e-06
LANES = 128
TILE = 256
F32 = jnp.float32
BF16 = jnp.bfloat16


def dot_nt(x, w):
    return lax.dot_general(x, w, (((1,), (1,)), ((), ())), preferred_element_type=F32)


def dot_nn(x, w):
    return lax.dot_general(x, w, (((1,), (0,)), ((), ())), preferred_element_type=F32)


def kernel(
    n_view, rows, cols, chans,
    lat_hbm, gain_hbm, shift_hbm, w1_hbm, b1_hbm, w2_hbm, b2_hbm,
    out_ref,
    lat, small, w1, gt, w2, fold, act, vbuf, mbuf, mx, lhs_u, part, wide, edge, raised, stat, stat_in,
    lat_sem, small_sem, w1_sem, w2_sem, halo_send, halo_recv, stat_send, stat_recv, ready, paired,
):
    me = lax.axis_index("view")
    slabs = H_LAT // rows
    assert slabs == 4
    views = n_view // slabs
    slab = me // views
    own = rows * cols
    has_up = slab > 0
    has_down = slab < slabs - 1

    barrier = pltpu.get_barrier_semaphore()

    hub = n_view - 2
    above, below = me - views, me + views
    first, second, third, last = slab == 0, slab == 1, slab == 2, slab == 3
    between = jnp.logical_or(second, third)
    rest = n_view - views
    unrolled = n_view <= 16

    def signal(to, carry=0):
        @pl.when(to != me)
        def _():
            pl.semaphore_signal(barrier, inc=1, device_id={"view": to})
        return carry

    def greet():
        lax.fori_loop(rest, n_view, signal, 0, unroll=unrolled)

        @pl.when(second)
        def _():
            signal(above)
            signal(below)

        @pl.when(first)
        def _():
            lax.fori_loop(views, rest, signal, 0, unroll=unrolled)

    def spread_word():
        @pl.when(me == hub)
        def _():
            pl.semaphore_wait(barrier, n_view - 1)

            def tell(to, carry):
                pl.semaphore_signal(ready, inc=1, device_id={"view": to})
                return carry

            lax.fori_loop(0, rest, tell, 0, unroll=unrolled)

    lat_rows = 1

    def lat_copy(i):
        some = pl.ds(i * lat_rows, lat_rows)
        return pltpu.make_async_copy(lat_hbm.at[some], lat.at[pl.ds(2 + i * lat_rows, lat_rows)], lat_sem.at[i])

    def small_copy(i):
        ref = (gain_hbm, shift_hbm, b1_hbm, b2_hbm)[i]
        return pltpu.make_async_copy(ref, small.at[i], small_sem)

    def w1_copy(t):
        return pltpu.make_async_copy(w1_hbm.at[t], w1.at[t], w1_sem.at[t // 5])

    def w2_copy(t):
        return pltpu.make_async_copy(w2_hbm.at[t], w2.at[t], w2_sem)

    for i in range(rows):
        lat_copy(i).start()
    greet()
    spread_word()
    for t in range(9):
        w1_copy(t).start(priority=1)
    for i in range(4):
        small_copy(i).start(priority=1)

    tiles = chans // TILE
    eye = (
        lax.broadcasted_iota(jnp.int32, (TILE, TILE), 0) == lax.broadcasted_iota(jnp.int32, (TILE, TILE), 1)
    ).astype(F32).astype(BF16)

    def prepare(j, carry):
        k0 = pl.multiple_of(j // tiles * TILE, TILE)
        n0 = pl.multiple_of(lax.rem(j, tiles) * TILE, TILE)
        for s in range(3):
            for k, r in ((0, 0), (3, 2)):
                g = w1[3 * r + s, pl.ds(n0, TILE), pl.ds(k0, TILE)]
                gt[k, s, pl.ds(k0, TILE), pl.ds(n0, TILE)] = dot_nt(eye, g).astype(BF16)
            for a in range(0, TILE, LANES):
                for b in range(0, TILE, LANES):
                    n_at, k_at = pl.ds(n0 + a, LANES), pl.ds(k0 + b, LANES)
                    h = [w1[3 * r + s, n_at, k_at].astype(F32) for r in range(3)]
                    even = (h[0] + h[2]) * 0.5
                    odd = h[1] * 0.5
                    gt[1, s, k_at, n_at] = (even + odd).astype(BF16).T
                    gt[2, s, k_at, n_at] = (even - odd).astype(BF16).T
        return carry

    def prepare_all():
        pltpu.make_async_copy(w1.at[pl.ds(0, 5)], w1.at[pl.ds(0, 5)], w1_sem.at[0]).wait()
        for t in range(9):
            w2_copy(t).start(priority=1)
        pltpu.make_async_copy(w1.at[pl.ds(5, 4)], w1.at[pl.ds(5, 4)], w1_sem.at[1]).wait()
        lax.fori_loop(0, tiles * tiles, prepare, 0)

    sums = jnp.zeros((8, chans), F32)
    squares = jnp.zeros((8, chans), F32)
    for i in range(rows):
        if i % lat_rows == 0:
            lat_copy(i // lat_rows).wait()
        x = lat[2 + i].astype(F32).reshape(cols // 8, 8, chans)
        sums = sums + jnp.sum(x, axis=0)
        squares = squares + jnp.sum(x * x, axis=0)
    sums = jnp.sum(sums, axis=0, keepdims=True)
    squares = jnp.sum(squares, axis=0, keepdims=True)
    blocks = chans // LANES
    stat[...] = jnp.concatenate(
        [v[:, k * LANES : (k + 1) * LANES] for v in (sums, squares) for k in range(blocks)], axis=0
    )

    up_copy = pltpu.make_async_remote_copy(
        src_ref=lat.at[pl.ds(2, 2)], dst_ref=lat.at[pl.ds(rows + 2, 2)],
        send_sem=halo_send.at[0], recv_sem=halo_recv.at[0],
        device_id={"view": jnp.maximum(above, 0)},
    )
    down_copy = pltpu.make_async_remote_copy(
        src_ref=lat.at[pl.ds(rows, 2)], dst_ref=lat.at[pl.ds(0, 2)],
        send_sem=halo_send.at[1], recv_sem=halo_recv.at[1],
        device_id={"view": jnp.minimum(below, n_view - 1)},
    )
    own_up = pltpu.make_async_copy(lat_hbm.at[pl.ds(0, 2)], lat.at[pl.ds(0, 2)], halo_recv.at[1])
    own_down = pltpu.make_async_copy(lat_hbm.at[pl.ds(0, 2)], lat.at[pl.ds(rows + 2, 2)], halo_recv.at[0])

    def send_halos(*pairs):
        for when, copy in pairs:
            @pl.when(when)
            def _():
                copy.start()

    def send_stat(to, carry):
        @pl.when(to != me)
        def _():
            slot = lax.rem(to - me + n_view, n_view) - 1
            pltpu.make_async_remote_copy(
                src_ref=stat, dst_ref=stat_in.at[slot], send_sem=stat_send, recv_sem=stat_recv,
                device_id={"view": to},
            ).start()
        return carry

    @pl.when(first)
    def _():
        pl.semaphore_wait(barrier, 1)

    @pl.when(third)
    def _():
        pl.semaphore_wait(barrier, views + 1)
        pl.semaphore_signal(paired, inc=1, device_id={"view": above})

    @pl.when(second)
    def _():
        pl.semaphore_wait(barrier, views)

    @pl.when(between)
    def _():
        lax.fori_loop(0, views, send_stat, 0, unroll=unrolled)

    send_halos((first, own_up), (first, down_copy), (between, up_copy))

    @pl.when(second)
    def _():
        pl.semaphore_wait(paired, 1)

    send_halos((second, down_copy))

    @pl.when(first)
    def _():
        prepare_all()

    @pl.when(jnp.logical_not(last))
    def _():
        pl.semaphore_wait(ready, 1)

    @pl.when(jnp.logical_and(last, me != hub))
    def _():
        pl.semaphore_wait(barrier, n_view - 1)

    @pl.when(jnp.logical_not(between))
    def _():
        lax.fori_loop(0, views, send_stat, 0, unroll=unrolled)

    lax.fori_loop(views, n_view, send_stat, 0, unroll=unrolled)
    send_halos(
        (last, up_copy), (third, down_copy), (last, own_down)
    )

    @pl.when(has_up)
    def _():
        prepare_all()

    zeros = jnp.zeros((edge.shape[1], 8, LANES), F32)

    def clear(k, carry):
        edge[k, :, pl.ds(0, 8)] = zeros
        edge[k, :, pl.ds(cols + 8, 8)] = zeros
        return carry

    lax.fori_loop(0, edge.shape[0], clear, 0)
    pltpu.make_async_copy(w2, w2, w2_sem).wait()

    def fold_tile(j, carry):
        k0 = pl.multiple_of(j // tiles * TILE, TILE)
        n0 = pl.multiple_of(lax.rem(j, tiles) * TILE, TILE)
        for k, t in enumerate((0, 2, 6, 8)):
            g = w2[t, pl.ds(n0, TILE), pl.ds(k0, TILE)]
            fold[5 + k, pl.ds(k0, TILE), pl.ds(n0, TILE)] = dot_nt(eye, g).astype(BF16)
        for a in range(0, TILE, LANES):
            for b in range(0, TILE, LANES):
                n_at, k_at = pl.ds(n0 + a, LANES), pl.ds(k0 + b, LANES)

                def add(*taps):
                    terms = [w2[t, n_at, k_at].astype(F32) for t in taps]
                    return terms[0] + terms[1] + terms[2]

                def put(i, v):
                    fold[i, k_at, n_at] = v.astype(BF16).T

                put(3, add(0, 1, 2))
                put(4, add(6, 7, 8))
                left = add(0, 3, 6)
                put(1, left)
                right = add(2, 5, 8)
                put(2, right)
                put(0, left + add(1, 4, 7) + right)
        return carry

    lax.fori_loop(0, tiles * tiles, fold_tile, 0)
    pltpu.make_async_copy(small, small, small_sem).wait()

    def raise_row(i, carry):
        raised[i] = lat[2 + i].astype(F32) + small[2]
        return carry

    lax.fori_loop(0, rows, raise_row, 0)

    same = (
        lax.broadcasted_iota(jnp.int32, (LANES, LANES), 0) // (chans // GROUPS)
        == lax.broadcasted_iota(jnp.int32, (LANES, LANES), 1) // (chans // GROUPS)
    ).astype(F32).astype(BF16)

    pltpu.make_async_copy(stat_in, stat_in, stat_recv).wait()

    total = stat[...] + jnp.sum(stat_in[...], axis=0)
    high = total.astype(BF16).astype(F32)
    rest = total - high
    middle = rest.astype(BF16).astype(F32)
    low = rest - middle
    parts = jnp.concatenate([high, middle, low, jnp.zeros_like(low)], axis=0).astype(BF16)
    sized = dot_nn(parts, same)
    n_stat = 2 * blocks
    total = sized[:n_stat] + sized[n_stat : 2 * n_stat] + sized[2 * n_stat : 3 * n_stat]
    entries = float(own * (chans // GROUPS) * n_view)
    mean = total[:blocks] * (1.0 / entries)
    var = total[blocks:] * (1.0 / entries) - mean * mean
    inv = lax.rsqrt(var + EPSILON)

    def one_row(v):
        return jnp.concatenate([v[k : k + 1] for k in range(blocks)], axis=1)

    scale = one_row(inv) * small[0]
    offset = small[1] - one_row(mean) * scale
    half_scale = scale * 0.5
    half_offset = offset * 0.5

    groups = range(chans // LANES)

    def beside(slot, g, x):
        edge[slot, g, pl.ds(8, cols)] = x
        return edge[slot, g, pl.ds(7, cols)], edge[slot, g, pl.ds(9, cols)]

    def activate(i):
        for g in groups:
            lanes = pl.ds(g * LANES, LANES)
            side = slice(g * LANES, (g + 1) * LANES)
            h = lat[i, :, lanes].astype(F32) * half_scale[:, side] + half_offset[:, side]
            a = h + h * jnp.tanh(h)
            if i < 2:
                a = jnp.where(has_up, a, 0.0)
            if i >= rows + 2:
                a = jnp.where(has_down, a, 0.0)
            left, right = beside(i, g, a)
            act[0, i, :, lanes] = left.astype(BF16)
            act[1, i, :, lanes] = a.astype(BF16)
            act[2, i, :, lanes] = right.astype(BF16)

    pairs = list(range(rows // 2 + 1))
    place = {p: p for p in pairs}

    def arrange(k, pairs):
        a, b = ((0, 2), (1, 2), (2, 1), (1, 3))[k]
        for p in pairs:
            at = pl.ds(place[p] * cols, cols)
            for s in range(3):
                x, y = act[s, 2 * p + a], act[s, 2 * p + b]
                vbuf[k, s, at] = x + y if k == 1 else x - y

    def products(n, k, pairs):
        at = pl.ds(place[pairs[0]] * cols, len(pairs) * cols)
        lanes = pl.ds(n * TILE, TILE)
        terms = [dot_nn(vbuf[k, s, at], gt[k, s, :, lanes]) for s in range(3)]
        mbuf[k, at, lanes] = terms[0] + terms[1] + terms[2]

    bias1 = small[2]

    def mix(n, i):
        p, odd = i // 2, i % 2
        at = pl.ds(place[p] * cols, cols)
        for g in groups[n * TILE // LANES : (n + 1) * TILE // LANES]:
            lanes = pl.ds(g * LANES, LANES)
            v = [mbuf[k, at, lanes] for k in ((1, 2, 3) if odd else (0, 1, 2))]
            conv = v[0] - v[1] - v[2] if odd else v[0] + v[1] + v[2]
            if 1 <= i <= rows:
                m = raised[i - 1, :, lanes] + conv
            else:
                m = lat[i + 1, :, lanes].astype(F32) + conv + bias1[:, g * LANES : (g + 1) * LANES]
            if i == 0:
                m = jnp.where(has_up, m, 0.0)
            if i == rows + 1:
                m = jnp.where(has_down, m, 0.0)
            narrow = m.astype(BF16)
            m = narrow.astype(F32)
            to = pl.ds(i * cols, cols)
            left, right = beside(rows + 4 + i, g, m)
            mx[0, to, lanes] = narrow
            mx[1, to, lanes] = left.astype(BF16) - narrow
            mx[2, to, lanes] = right.astype(BF16) - narrow

    def rise_of(n, j):
        lanes = pl.ds(n * TILE, TILE)
        here, below = pl.ds(j * cols, cols), pl.ds((j + 1) * cols, cols)
        for s in range(3):
            lhs_u[s, here, lanes] = mx[s, below, lanes] - mx[s, here, lanes]

    width = TILE
    bias2 = small[3]

    def take(ref, s, pieces):
        return jnp.concatenate([ref[s, pl.ds(a * cols, b * cols)] for a, b in pieces], axis=0)

    def level(n, pieces):
        lanes = pl.ds(n * width, width)
        mine = [(a + 1, b) for a, b in pieces]
        base = dot_nn(take(mx, 0, mine), fold[0, :, lanes]) + bias2[:, n * width : (n + 1) * width]
        for q in range(2):
            both = base + dot_nn(take(mx, 1 + q, mine), fold[1 + q, :, lanes])
            done = 0
            for a, b in pieces:
                part[n, q, pl.ds(a * cols, b * cols)] = both[done * cols : (done + b) * cols]
                done += b

    def finish(n, p, pieces):
        lanes = pl.ds(n * width, width)
        mine = [(a + p, b) for a, b in pieces]
        rise = dot_nn(take(lhs_u, 0, mine), fold[3 + p, :, lanes])
        for q in range(2):
            term = rise + dot_nn(take(lhs_u, 1 + q, mine), fold[5 + 2 * p + q, :, lanes])
            done = 0
            for a, b in pieces:
                for i in range(a, a + b):
                    for g in range(width // LANES):
                        x = part[n, q, pl.ds(i * cols, cols), pl.ds(g * LANES, LANES)]
                        y = term[done * cols : (done + 1) * cols, g * LANES : (g + 1) * LANES]
                        wide[g, pl.ds((p * rows + i) * 2 * cols + q, cols, 2), :] = x + y if p else x - y
                    done += 1
        for a, b in pieces:
            for i in range(a, a + b):
                for g in range(width // LANES):
                    tile = wide[g, pl.ds((p * rows + i) * 2 * cols, 2 * cols), :].astype(BF16)
                    out_ref[i, p, :, pl.ds(n * width + g * LANES, LANES)] = tile

    columns = range(chans // width)

    for i in range(2, 6, 2):
        activate(i)

    own_up.wait()
    own_down.wait()
    for i in (0, *range(6, rows + 4, 2)):
        activate(i)
    arrange(0, pairs)
    for n in columns:
        products(n, 0, pairs)
    for i in range(1, rows + 4, 2):
        activate(i)
    for n in columns:
        for k in (3, 1, 2):
            if n == 0:
                arrange(k, pairs)
            products(n, k, pairs)
        if n:
            for i in range(rows + 2):
                mix(n - 1, i)
    for i in range(rows + 2):
        mix(columns[-1], i)
    for n in columns:
        for j in range(rows + 1):
            rise_of(n, j)
    for n in columns:
        level(n, [(0, rows)])
        for p in range(2):
            finish(n, p, [(0, rows)])

    pltpu.make_async_copy(stat_in, stat_in, stat_send).wait()

    @pl.when(has_up)
    def _():
        up_copy.wait_send()

    @pl.when(has_down)
    def _():
        down_copy.wait_send()


def per_device(n_view, latents, norm_gain, norm_shift, w_first, bias_first, w_second, bias_second):
    rows, cols, chans = latents.shape
    own = rows * cols
    flat = lambda w: jnp.transpose(w, (1, 2, 0, 3)).reshape(9, chans, chans)
    row = lambda v: v.reshape(1, chans)
    hbm = pl.BlockSpec(memory_space=pl.ANY)
    n_stat = 2 * chans // LANES
    out = pl.pallas_call(
        functools.partial(kernel, n_view, rows, cols, chans),
        out_shape=pltpu.VMEM((rows, 2, 2 * cols, chans), BF16),
        in_specs=[hbm] * 7,
        out_specs=pl.BlockSpec(memory_space=pltpu.VMEM),
        scratch_shapes=[
            pltpu.VMEM((rows + 4, cols, chans), BF16),
            pltpu.VMEM((4, 1, chans), F32),
            pltpu.VMEM((9, chans, chans), BF16),
            pltpu.VMEM((4, 3, chans, chans), BF16),
            pltpu.VMEM((9, chans, chans), BF16),
            pltpu.VMEM((9, chans, chans), BF16),
            pltpu.VMEM((3, rows + 4, cols, chans), BF16),
            pltpu.VMEM((4, 3, (rows // 2 + 1) * cols, chans), BF16),
            pltpu.VMEM((4, (rows // 2 + 1) * cols, chans), F32),
            pltpu.VMEM((3, own + 2 * cols, chans), BF16),
            pltpu.VMEM((3, own + cols, chans), BF16),
            pltpu.VMEM((chans // TILE, 2, own, TILE), F32),
            pltpu.VMEM((TILE // LANES, own * 4, LANES), F32),
            pltpu.VMEM((2 * rows + 6, chans // LANES, cols + 16, LANES), F32),
            pltpu.VMEM((rows, cols, chans), F32),
            pltpu.VMEM((n_stat, LANES), F32),
            pltpu.VMEM((n_view - 1, n_stat, LANES), F32),
            pltpu.SemaphoreType.DMA((rows,)),
            pltpu.SemaphoreType.DMA,
            pltpu.SemaphoreType.DMA((2,)),
            pltpu.SemaphoreType.DMA,
            pltpu.SemaphoreType.DMA((2,)),
            pltpu.SemaphoreType.DMA((2,)),
            pltpu.SemaphoreType.DMA,
            pltpu.SemaphoreType.DMA,
            pltpu.SemaphoreType.REGULAR,
            pltpu.SemaphoreType.REGULAR,
        ],
        compiler_params=pltpu.CompilerParams(
            collective_id=0, has_side_effects=True, vmem_limit_bytes=60 * 1024 * 1024
        ),
    )(
        latents, row(norm_gain), row(norm_shift), flat(w_first), row(bias_first), flat(w_second),
        row(bias_second),
    )
    return out.reshape(2 * rows, 2 * cols, chans)


def solution(mesh):
    placed = (P(("scene", "view"), None, None), P(), P(), P(), P(), P(), P())
    return jax.shard_map(
        functools.partial(per_device, mesh.shape["view"]),
        mesh=mesh,
        in_specs=placed,
        out_specs=P(("scene", "view"), None, None),
        check_vma=False,
    )
```

```python
import functools

import jax
import jax.numpy as jnp
from jax import lax
from jax.experimental import pallas as pl
from jax.experimental.pallas import tpu as pltpu
from jax.sharding import PartitionSpec as P

GROUPS = 32
H_LAT = 32
EPSILON = 1e-06
LANES = 128
TILE = 256
F32 = jnp.float32
BF16 = jnp.bfloat16


def dot_nt(x, w):
    return lax.dot_general(x, w, (((1,), (1,)), ((), ())), preferred_element_type=F32)


def dot_nn(x, w):
    return lax.dot_general(x, w, (((1,), (0,)), ((), ())), preferred_element_type=F32)


def kernel(
    n_view, rows, cols, chans,
    lat_hbm, gain_hbm, shift_hbm, w1_hbm, b1_hbm, w2_hbm, b2_hbm,
    out_ref,
    lat, small, w1, gt, w2, fold, act, vbuf, mbuf, mx, lhs_u, part, wide, edge, raised, stat, stat_in,
    lat_sem, small_sem, w1_sem, w2_sem, halo_send, halo_recv, stat_send, stat_recv, ready, paired,
):
    me = lax.axis_index("view")
    slabs = H_LAT // rows
    assert slabs == 4
    views = n_view // slabs
    slab = me // views
    own = rows * cols
    has_up = slab > 0
    has_down = slab < slabs - 1

    barrier = pltpu.get_barrier_semaphore()

    hub = n_view - 2
    above, below = me - views, me + views
    first, second, third, last = slab == 0, slab == 1, slab == 2, slab == 3
    between = jnp.logical_or(second, third)
    rest = n_view - views
    unrolled = n_view <= 16

    def signal(to, carry=0):
        @pl.when(to != me)
        def _():
            pl.semaphore_signal(barrier, inc=1, device_id={"view": to})
        return carry

    def greet():
        lax.fori_loop(rest, n_view, signal, 0, unroll=unrolled)

        @pl.when(second)
        def _():
            signal(above)
            signal(below)

        @pl.when(first)
        def _():
            lax.fori_loop(views, rest, signal, 0, unroll=unrolled)

    def spread_word():
        @pl.when(me == hub)
        def _():
            pl.semaphore_wait(barrier, n_view - 1)

            def tell(to, carry):
                pl.semaphore_signal(ready, inc=1, device_id={"view": to})
                return carry

            lax.fori_loop(0, rest, tell, 0, unroll=unrolled)

    lat_rows = 1

    def lat_copy(i):
        some = pl.ds(i * lat_rows, lat_rows)
        return pltpu.make_async_copy(lat_hbm.at[some], lat.at[pl.ds(2 + i * lat_rows, lat_rows)], lat_sem.at[i])

    def small_copy(i):
        ref = (gain_hbm, shift_hbm, b1_hbm, b2_hbm)[i]
        return pltpu.make_async_copy(ref, small.at[i], small_sem)

    def w1_copy(t):
        return pltpu.make_async_copy(w1_hbm.at[t], w1.at[t], w1_sem.at[t // 5])

    def w2_copy(t):
        return pltpu.make_async_copy(w2_hbm.at[t], w2.at[t], w2_sem)

    for i in range(rows):
        lat_copy(i).start()
    greet()
    spread_word()
    for t in range(9):
        w1_copy(t).start(priority=1)
    for i in range(4):
        small_copy(i).start(priority=1)

    tiles = chans // TILE
    eye = (
        lax.broadcasted_iota(jnp.int32, (TILE, TILE), 0) == lax.broadcasted_iota(jnp.int32, (TILE, TILE), 1)
    ).astype(F32).astype(BF16)

    def prepare(j, carry):
        k0 = pl.multiple_of(j // tiles * TILE, TILE)
        n0 = pl.multiple_of(lax.rem(j, tiles) * TILE, TILE)
        for s in range(3):
            for k, r in ((0, 0), (3, 2)):
                g = w1[3 * r + s, pl.ds(n0, TILE), pl.ds(k0, TILE)]
                gt[k, s, pl.ds(k0, TILE), pl.ds(n0, TILE)] = dot_nt(eye, g).astype(BF16)
            for a in range(0, TILE, LANES):
                for b in range(0, TILE, LANES):
                    n_at, k_at = pl.ds(n0 + a, LANES), pl.ds(k0 + b, LANES)
                    h = [w1[3 * r + s, n_at, k_at].astype(F32) for r in range(3)]
                    even = (h[0] + h[2]) * 0.5
                    odd = h[1] * 0.5
                    gt[1, s, k_at, n_at] = (even + odd).astype(BF16).T
                    gt[2, s, k_at, n_at] = (even - odd).astype(BF16).T
        return carry

    def prepare_all():
        pltpu.make_async_copy(w1.at[pl.ds(0, 5)], w1.at[pl.ds(0, 5)], w1_sem.at[0]).wait()
        for t in range(9):
            w2_copy(t).start(priority=1)
        pltpu.make_async_copy(w1.at[pl.ds(5, 4)], w1.at[pl.ds(5, 4)], w1_sem.at[1]).wait()
        lax.fori_loop(0, tiles * tiles, prepare, 0)

    sums = jnp.zeros((8, chans), F32)
    squares = jnp.zeros((8, chans), F32)
    for i in range(rows):
        if i % lat_rows == 0:
            lat_copy(i // lat_rows).wait()
        x = lat[2 + i].astype(F32).reshape(cols // 8, 8, chans)
        sums = sums + jnp.sum(x, axis=0)
        squares = squares + jnp.sum(x * x, axis=0)
    sums = jnp.sum(sums, axis=0, keepdims=True)
    squares = jnp.sum(squares, axis=0, keepdims=True)
    blocks = chans // LANES
    stat[...] = jnp.concatenate(
        [v[:, k * LANES : (k + 1) * LANES] for v in (sums, squares) for k in range(blocks)], axis=0
    )

    up_copy = pltpu.make_async_remote_copy(
        src_ref=lat.at[pl.ds(2, 2)], dst_ref=lat.at[pl.ds(rows + 2, 2)],
        send_sem=halo_send.at[0], recv_sem=halo_recv.at[0],
        device_id={"view": jnp.maximum(above, 0)},
    )
    down_copy = pltpu.make_async_remote_copy(
        src_ref=lat.at[pl.ds(rows, 2)], dst_ref=lat.at[pl.ds(0, 2)],
        send_sem=halo_send.at[1], recv_sem=halo_recv.at[1],
        device_id={"view": jnp.minimum(below, n_view - 1)},
    )
    own_up = pltpu.make_async_copy(lat_hbm.at[pl.ds(0, 2)], lat.at[pl.ds(0, 2)], halo_recv.at[1])
    own_down = pltpu.make_async_copy(lat_hbm.at[pl.ds(0, 2)], lat.at[pl.ds(rows + 2, 2)], halo_recv.at[0])

    def send_halos(*pairs):
        for when, copy in pairs:
            @pl.when(when)
            def _():
                copy.start()

    def send_stat(to, carry):
        @pl.when(to != me)
        def _():
            slot = lax.rem(to - me + n_view, n_view) - 1
            pltpu.make_async_remote_copy(
                src_ref=stat, dst_ref=stat_in.at[slot], send_sem=stat_send, recv_sem=stat_recv,
                device_id={"view": to},
            ).start()
        return carry

    @pl.when(first)
    def _():
        pl.semaphore_wait(barrier, 1)

    @pl.when(third)
    def _():
        pl.semaphore_wait(barrier, views + 1)
        pl.semaphore_signal(paired, inc=1, device_id={"view": above})

    @pl.when(second)
    def _():
        pl.semaphore_wait(barrier, views)

    @pl.when(between)
    def _():
        lax.fori_loop(0, views, send_stat, 0, unroll=unrolled)

    send_halos((first, own_up), (first, down_copy), (between, up_copy))

    @pl.when(second)
    def _():
        pl.semaphore_wait(paired, 1)

    send_halos((second, down_copy))

    @pl.when(first)
    def _():
        prepare_all()

    @pl.when(jnp.logical_not(last))
    def _():
        pl.semaphore_wait(ready, 1)

    @pl.when(jnp.logical_and(last, me != hub))
    def _():
        pl.semaphore_wait(barrier, n_view - 1)

    @pl.when(jnp.logical_not(between))
    def _():
        lax.fori_loop(0, views, send_stat, 0, unroll=unrolled)

    lax.fori_loop(views, n_view, send_stat, 0, unroll=unrolled)
    send_halos(
        (last, up_copy), (third, down_copy), (last, own_down)
    )

    @pl.when(has_up)
    def _():
        prepare_all()

    zeros = jnp.zeros((edge.shape[1], 8, LANES), F32)

    def clear(k, carry):
        edge[k, :, pl.ds(0, 8)] = zeros
        edge[k, :, pl.ds(cols + 8, 8)] = zeros
        return carry

    lax.fori_loop(0, edge.shape[0], clear, 0)
    pltpu.make_async_copy(w2, w2, w2_sem).wait()

    def fold_tile(j, carry):
        k0 = pl.multiple_of(j // tiles * TILE, TILE)
        n0 = pl.multiple_of(lax.rem(j, tiles) * TILE, TILE)
        for k, t in enumerate((0, 2, 6, 8)):
            g = w2[t, pl.ds(n0, TILE), pl.ds(k0, TILE)]
            fold[5 + k, pl.ds(k0, TILE), pl.ds(n0, TILE)] = dot_nt(eye, g).astype(BF16)
        for a in range(0, TILE, LANES):
            for b in range(0, TILE, LANES):
                n_at, k_at = pl.ds(n0 + a, LANES), pl.ds(k0 + b, LANES)

                def add(*taps):
                    terms = [w2[t, n_at, k_at].astype(F32) for t in taps]
                    return terms[0] + terms[1] + terms[2]

                def put(i, v):
                    fold[i, k_at, n_at] = v.astype(BF16).T

                put(3, add(0, 1, 2))
                put(4, add(6, 7, 8))
                left = add(0, 3, 6)
                put(1, left)
                right = add(2, 5, 8)
                put(2, right)
                put(0, left + add(1, 4, 7) + right)
        return carry

    lax.fori_loop(0, tiles * tiles, fold_tile, 0)
    pltpu.make_async_copy(small, small, small_sem).wait()

    def raise_row(i, carry):
        raised[i] = lat[2 + i].astype(F32) + small[2]
        return carry

    lax.fori_loop(0, rows, raise_row, 0)

    same = (
        lax.broadcasted_iota(jnp.int32, (LANES, LANES), 0) // (chans // GROUPS)
        == lax.broadcasted_iota(jnp.int32, (LANES, LANES), 1) // (chans // GROUPS)
    ).astype(F32).astype(BF16)

    pltpu.make_async_copy(stat_in, stat_in, stat_recv).wait()

    total = stat[...] + jnp.sum(stat_in[...], axis=0)
    high = total.astype(BF16).astype(F32)
    rest = total - high
    middle = rest.astype(BF16).astype(F32)
    low = rest - middle
    parts = jnp.concatenate([high, middle, low, jnp.zeros_like(low)], axis=0).astype(BF16)
    sized = dot_nn(parts, same)
    n_stat = 2 * blocks
    total = sized[:n_stat] + sized[n_stat : 2 * n_stat] + sized[2 * n_stat : 3 * n_stat]
    entries = float(own * (chans // GROUPS) * n_view)
    mean = total[:blocks] * (1.0 / entries)
    var = total[blocks:] * (1.0 / entries) - mean * mean
    inv = lax.rsqrt(var + EPSILON)

    def one_row(v):
        return jnp.concatenate([v[k : k + 1] for k in range(blocks)], axis=1)

    scale = one_row(inv) * small[0]
    offset = small[1] - one_row(mean) * scale
    half_scale = scale * 0.5
    half_offset = offset * 0.5

    groups = range(chans // LANES)

    def beside(slot, g, x):
        edge[slot, g, pl.ds(8, cols)] = x
        return edge[slot, g, pl.ds(7, cols)], edge[slot, g, pl.ds(9, cols)]

    def activate(i):
        for g in groups:
            lanes = pl.ds(g * LANES, LANES)
            side = slice(g * LANES, (g + 1) * LANES)
            h = lat[i, :, lanes].astype(F32) * half_scale[:, side] + half_offset[:, side]
            a = h + h * jnp.tanh(h)
            if i < 2:
                a = jnp.where(has_up, a, 0.0)
            if i >= rows + 2:
                a = jnp.where(has_down, a, 0.0)
            left, right = beside(i, g, a)
            act[0, i, :, lanes] = left.astype(BF16)
            act[1, i, :, lanes] = a.astype(BF16)
            act[2, i, :, lanes] = right.astype(BF16)

    pairs = list(range(rows // 2 + 1))
    place = {p: p for p in pairs}

    def arrange(k, pairs):
        a, b = ((0, 2), (1, 2), (2, 1), (1, 3))[k]
        for p in pairs:
            at = pl.ds(place[p] * cols, cols)
            for s in range(3):
                x, y = act[s, 2 * p + a], act[s, 2 * p + b]
                vbuf[k, s, at] = x + y if k == 1 else x - y

    def products(n, k, pairs):
        at = pl.ds(place[pairs[0]] * cols, len(pairs) * cols)
        lanes = pl.ds(n * TILE, TILE)
        terms = [dot_nn(vbuf[k, s, at], gt[k, s, :, lanes]) for s in range(3)]
        mbuf[k, at, lanes] = terms[0] + terms[1] + terms[2]

    bias1 = small[2]

    def mix(n, i):
        p, odd = i // 2, i % 2
        at = pl.ds(place[p] * cols, cols)
        for g in groups[n * TILE // LANES : (n + 1) * TILE // LANES]:
            lanes = pl.ds(g * LANES, LANES)
            v = [mbuf[k, at, lanes] for k in ((1, 2, 3) if odd else (0, 1, 2))]
            conv = v[0] - v[1] - v[2] if odd else v[0] + v[1] + v[2]
            if 1 <= i <= rows:
                m = raised[i - 1, :, lanes] + conv
            else:
                m = lat[i + 1, :, lanes].astype(F32) + conv + bias1[:, g * LANES : (g + 1) * LANES]
            if i == 0:
                m = jnp.where(has_up, m, 0.0)
            if i == rows + 1:
                m = jnp.where(has_down, m, 0.0)
            narrow = m.astype(BF16)
            m = narrow.astype(F32)
            to = pl.ds(i * cols, cols)
            left, right = beside(rows + 4 + i, g, m)
            mx[0, to, lanes] = narrow
            mx[1, to, lanes] = left.astype(BF16) - narrow
            mx[2, to, lanes] = right.astype(BF16) - narrow

    def rise_of(n, j):
        lanes = pl.ds(n * TILE, TILE)
        here, below = pl.ds(j * cols, cols), pl.ds((j + 1) * cols, cols)
        for s in range(3):
            lhs_u[s, here, lanes] = mx[s, below, lanes] - mx[s, here, lanes]

    width = TILE
    bias2 = small[3]

    def take(ref, s, pieces):
        return jnp.concatenate([ref[s, pl.ds(a * cols, b * cols)] for a, b in pieces], axis=0)

    def level(n, pieces):
        lanes = pl.ds(n * width, width)
        mine = [(a + 1, b) for a, b in pieces]
        base = dot_nn(take(mx, 0, mine), fold[0, :, lanes]) + bias2[:, n * width : (n + 1) * width]
        for q in range(2):
            both = base + dot_nn(take(mx, 1 + q, mine), fold[1 + q, :, lanes])
            done = 0
            for a, b in pieces:
                part[n, q, pl.ds(a * cols, b * cols)] = both[done * cols : (done + b) * cols]
                done += b

    def finish(n, p, pieces):
        lanes = pl.ds(n * width, width)
        mine = [(a + p, b) for a, b in pieces]
        rise = dot_nn(take(lhs_u, 0, mine), fold[3 + p, :, lanes])
        for q in range(2):
            term = rise + dot_nn(take(lhs_u, 1 + q, mine), fold[5 + 2 * p + q, :, lanes])
            done = 0
            for a, b in pieces:
                for i in range(a, a + b):
                    for g in range(width // LANES):
                        x = part[n, q, pl.ds(i * cols, cols), pl.ds(g * LANES, LANES)]
                        y = term[done * cols : (done + 1) * cols, g * LANES : (g + 1) * LANES]
                        wide[g, pl.ds((p * rows + i) * 2 * cols + q, cols, 2), :] = x + y if p else x - y
                    done += 1
        for a, b in pieces:
            for i in range(a, a + b):
                for g in range(width // LANES):
                    tile = wide[g, pl.ds((p * rows + i) * 2 * cols, 2 * cols), :].astype(BF16)
                    out_ref[i, p, :, pl.ds(n * width + g * LANES, LANES)] = tile

    columns = range(chans // width)

    for i in range(2, 4, 2):
        activate(i)

    own_up.wait()
    own_down.wait()
    for i in (0, *range(4, rows + 4, 2)):
        activate(i)
    arrange(0, pairs)
    for n in columns:
        products(n, 0, pairs)
    for i in range(1, rows + 4, 2):
        activate(i)
    for n in columns:
        for k in (3, 1, 2):
            if n == 0:
                arrange(k, pairs)
            products(n, k, pairs)
        if n:
            for i in range(rows + 2):
                mix(n - 1, i)
    for i in range(rows + 2):
        mix(columns[-1], i)
    for n in columns:
        for j in range(rows + 1):
            rise_of(n, j)
    for n in columns:
        level(n, [(0, rows)])
        for p in range(2):
            finish(n, p, [(0, rows)])

    pltpu.make_async_copy(stat_in, stat_in, stat_send).wait()

    @pl.when(has_up)
    def _():
        up_copy.wait_send()

    @pl.when(has_down)
    def _():
        down_copy.wait_send()


def per_device(n_view, latents, norm_gain, norm_shift, w_first, bias_first, w_second, bias_second):
    rows, cols, chans = latents.shape
    own = rows * cols
    flat = lambda w: jnp.transpose(w, (1, 2, 0, 3)).reshape(9, chans, chans)
    row = lambda v: v.reshape(1, chans)
    hbm = pl.BlockSpec(memory_space=pl.ANY)
    n_stat = 2 * chans // LANES
    out = pl.pallas_call(
        functools.partial(kernel, n_view, rows, cols, chans),
        out_shape=pltpu.VMEM((rows, 2, 2 * cols, chans), BF16),
        in_specs=[hbm] * 7,
        out_specs=pl.BlockSpec(memory_space=pltpu.VMEM),
        scratch_shapes=[
            pltpu.VMEM((rows + 4, cols, chans), BF16),
            pltpu.VMEM((4, 1, chans), F32),
            pltpu.VMEM((9, chans, chans), BF16),
            pltpu.VMEM((4, 3, chans, chans), BF16),
            pltpu.VMEM((9, chans, chans), BF16),
            pltpu.VMEM((9, chans, chans), BF16),
            pltpu.VMEM((3, rows + 4, cols, chans), BF16),
            pltpu.VMEM((4, 3, (rows // 2 + 1) * cols, chans), BF16),
            pltpu.VMEM((4, (rows // 2 + 1) * cols, chans), F32),
            pltpu.VMEM((3, own + 2 * cols, chans), BF16),
            pltpu.VMEM((3, own + cols, chans), BF16),
            pltpu.VMEM((chans // TILE, 2, own, TILE), F32),
            pltpu.VMEM((TILE // LANES, own * 4, LANES), F32),
            pltpu.VMEM((2 * rows + 6, chans // LANES, cols + 16, LANES), F32),
            pltpu.VMEM((rows, cols, chans), F32),
            pltpu.VMEM((n_stat, LANES), F32),
            pltpu.VMEM((n_view - 1, n_stat, LANES), F32),
            pltpu.SemaphoreType.DMA((rows,)),
            pltpu.SemaphoreType.DMA,
            pltpu.SemaphoreType.DMA((2,)),
            pltpu.SemaphoreType.DMA,
            pltpu.SemaphoreType.DMA((2,)),
            pltpu.SemaphoreType.DMA((2,)),
            pltpu.SemaphoreType.DMA,
            pltpu.SemaphoreType.DMA,
            pltpu.SemaphoreType.REGULAR,
            pltpu.SemaphoreType.REGULAR,
        ],
        compiler_params=pltpu.CompilerParams(
            collective_id=0, has_side_effects=True, vmem_limit_bytes=60 * 1024 * 1024
        ),
    )(
        latents, row(norm_gain), row(norm_shift), flat(w_first), row(bias_first), flat(w_second),
        row(bias_second),
    )
    return out.reshape(2 * rows, 2 * cols, chans)


def solution(mesh):
    placed = (P(("scene", "view"), None, None), P(), P(), P(), P(), P(), P())
    return jax.shard_map(
        functools.partial(per_device, mesh.shape["view"]),
        mesh=mesh,
        in_specs=placed,
        out_specs=P(("scene", "view"), None, None),
        check_vma=False,
    )
```

```python
import functools

import jax
import jax.numpy as jnp
from jax import lax
from jax.experimental import pallas as pl
from jax.experimental.pallas import tpu as pltpu
from jax.sharding import PartitionSpec as P

GROUPS = 32
H_LAT = 32
EPSILON = 1e-06
LANES = 128
TILE = 256
F32 = jnp.float32
BF16 = jnp.bfloat16


def dot_nt(x, w):
    return lax.dot_general(x, w, (((1,), (1,)), ((), ())), preferred_element_type=F32)


def dot_nn(x, w):
    return lax.dot_general(x, w, (((1,), (0,)), ((), ())), preferred_element_type=F32)


def kernel(
    n_view, rows, cols, chans,
    lat_hbm, gain_hbm, shift_hbm, w1_hbm, b1_hbm, w2_hbm, b2_hbm,
    out_ref,
    lat, small, w1, gt, w2, fold, act, vbuf, mbuf, mx, lhs_u, part, wide, edge, raised, stat, stat_in,
    lat_sem, small_sem, w1_sem, w2_sem, halo_send, halo_recv, stat_send, stat_recv, ready, paired,
):
    me = lax.axis_index("view")
    slabs = H_LAT // rows
    assert slabs == 4
    views = n_view // slabs
    slab = me // views
    own = rows * cols
    has_up = slab > 0
    has_down = slab < slabs - 1

    barrier = pltpu.get_barrier_semaphore()

    hub = n_view - 2
    above, below = me - views, me + views
    first, second, third, last = slab == 0, slab == 1, slab == 2, slab == 3
    between = jnp.logical_or(second, third)
    rest = n_view - views
    unrolled = n_view <= 16

    def signal(to, carry=0):
        @pl.when(to != me)
        def _():
            pl.semaphore_signal(barrier, inc=1, device_id={"view": to})
        return carry

    def greet():
        lax.fori_loop(rest, n_view, signal, 0, unroll=unrolled)

        @pl.when(second)
        def _():
            signal(above)
            signal(below)

        @pl.when(first)
        def _():
            lax.fori_loop(views, rest, signal, 0, unroll=unrolled)

    def spread_word():
        @pl.when(me == hub)
        def _():
            pl.semaphore_wait(barrier, n_view - 1)

            def tell(to, carry):
                pl.semaphore_signal(ready, inc=1, device_id={"view": to})
                return carry

            lax.fori_loop(0, rest, tell, 0, unroll=unrolled)

    lat_rows = 1

    def lat_copy(i):
        some = pl.ds(i * lat_rows, lat_rows)
        return pltpu.make_async_copy(lat_hbm.at[some], lat.at[pl.ds(2 + i * lat_rows, lat_rows)], lat_sem.at[i])

    def small_copy(i):
        ref = (gain_hbm, shift_hbm, b1_hbm, b2_hbm)[i]
        return pltpu.make_async_copy(ref, small.at[i], small_sem)

    def w1_copy(t):
        return pltpu.make_async_copy(w1_hbm.at[t], w1.at[t], w1_sem.at[t // 5])

    def w2_copy(t):
        return pltpu.make_async_copy(w2_hbm.at[t], w2.at[t], w2_sem)

    for i in range(rows):
        lat_copy(i).start()
    greet()
    spread_word()
    for t in range(9):
        w1_copy(t).start(priority=1)
    for i in range(4):
        small_copy(i).start(priority=1)

    tiles = chans // TILE
    eye = (
        lax.broadcasted_iota(jnp.int32, (TILE, TILE), 0) == lax.broadcasted_iota(jnp.int32, (TILE, TILE), 1)
    ).astype(F32).astype(BF16)

    def prepare(j, carry):
        k0 = pl.multiple_of(j // tiles * TILE, TILE)
        n0 = pl.multiple_of(lax.rem(j, tiles) * TILE, TILE)
        for s in range(3):
            for k, r in ((0, 0), (3, 2)):
                g = w1[3 * r + s, pl.ds(n0, TILE), pl.ds(k0, TILE)]
                gt[k, s, pl.ds(k0, TILE), pl.ds(n0, TILE)] = dot_nt(eye, g).astype(BF16)
            for a in range(0, TILE, LANES):
                for b in range(0, TILE, LANES):
                    n_at, k_at = pl.ds(n0 + a, LANES), pl.ds(k0 + b, LANES)
                    h = [w1[3 * r + s, n_at, k_at].astype(F32) for r in range(3)]
                    even = (h[0] + h[2]) * 0.5
                    odd = h[1] * 0.5
                    gt[1, s, k_at, n_at] = (even + odd).astype(BF16).T
                    gt[2, s, k_at, n_at] = (even - odd).astype(BF16).T
        return carry

    def prepare_all():
        pltpu.make_async_copy(w1.at[pl.ds(0, 5)], w1.at[pl.ds(0, 5)], w1_sem.at[0]).wait()
        for t in range(9):
            w2_copy(t).start(priority=1)
        pltpu.make_async_copy(w1.at[pl.ds(5, 4)], w1.at[pl.ds(5, 4)], w1_sem.at[1]).wait()
        lax.fori_loop(0, tiles * tiles, prepare, 0)

    sums = jnp.zeros((8, chans), F32)
    squares = jnp.zeros((8, chans), F32)
    for i in range(rows):
        if i % lat_rows == 0:
            lat_copy(i // lat_rows).wait()
        x = lat[2 + i].astype(F32).reshape(cols // 8, 8, chans)
        sums = sums + jnp.sum(x, axis=0)
        squares = squares + jnp.sum(x * x, axis=0)
    sums = jnp.sum(sums, axis=0, keepdims=True)
    squares = jnp.sum(squares, axis=0, keepdims=True)
    blocks = chans // LANES
    stat[...] = jnp.concatenate(
        [v[:, k * LANES : (k + 1) * LANES] for v in (sums, squares) for k in range(blocks)], axis=0
    )

    up_copy = pltpu.make_async_remote_copy(
        src_ref=lat.at[pl.ds(2, 2)], dst_ref=lat.at[pl.ds(rows + 2, 2)],
        send_sem=halo_send.at[0], recv_sem=halo_recv.at[0],
        device_id={"view": jnp.maximum(above, 0)},
    )
    down_copy = pltpu.make_async_remote_copy(
        src_ref=lat.at[pl.ds(rows, 2)], dst_ref=lat.at[pl.ds(0, 2)],
        send_sem=halo_send.at[1], recv_sem=halo_recv.at[1],
        device_id={"view": jnp.minimum(below, n_view - 1)},
    )
    own_up = pltpu.make_async_copy(lat_hbm.at[pl.ds(0, 2)], lat.at[pl.ds(0, 2)], halo_recv.at[1])
    own_down = pltpu.make_async_copy(lat_hbm.at[pl.ds(0, 2)], lat.at[pl.ds(rows + 2, 2)], halo_recv.at[0])

    def send_halos(*pairs):
        for when, copy in pairs:
            @pl.when(when)
            def _():
                copy.start()

    def send_stat(to, carry):
        @pl.when(to != me)
        def _():
            slot = lax.rem(to - me + n_view, n_view) - 1
            pltpu.make_async_remote_copy(
                src_ref=stat, dst_ref=stat_in.at[slot], send_sem=stat_send, recv_sem=stat_recv,
                device_id={"view": to},
            ).start()
        return carry

    @pl.when(first)
    def _():
        pl.semaphore_wait(barrier, 1)

    @pl.when(third)
    def _():
        pl.semaphore_wait(barrier, views + 1)
        pl.semaphore_signal(paired, inc=1, device_id={"view": above})

    @pl.when(second)
    def _():
        pl.semaphore_wait(barrier, views)

    @pl.when(between)
    def _():
        lax.fori_loop(0, views, send_stat, 0, unroll=unrolled)

    send_halos((first, own_up), (first, down_copy), (between, up_copy))

    @pl.when(second)
    def _():
        pl.semaphore_wait(paired, 1)

    send_halos((second, down_copy))

    @pl.when(first)
    def _():
        prepare_all()

    @pl.when(jnp.logical_not(last))
    def _():
        pl.semaphore_wait(ready, 1)

    @pl.when(jnp.logical_and(last, me != hub))
    def _():
        pl.semaphore_wait(barrier, n_view - 1)

    @pl.when(jnp.logical_not(between))
    def _():
        lax.fori_loop(0, views, send_stat, 0, unroll=unrolled)

    lax.fori_loop(views, n_view, send_stat, 0, unroll=unrolled)
    send_halos(
        (last, up_copy), (third, down_copy), (last, own_down)
    )

    @pl.when(has_up)
    def _():
        prepare_all()

    zeros = jnp.zeros((edge.shape[1], 8, LANES), F32)

    def clear(k, carry):
        edge[k, :, pl.ds(0, 8)] = zeros
        edge[k, :, pl.ds(cols + 8, 8)] = zeros
        return carry

    lax.fori_loop(0, edge.shape[0], clear, 0)
    pltpu.make_async_copy(w2, w2, w2_sem).wait()

    def fold_tile(j, carry):
        k0 = pl.multiple_of(j // tiles * TILE, TILE)
        n0 = pl.multiple_of(lax.rem(j, tiles) * TILE, TILE)
        for k, t in enumerate((0, 2, 6, 8)):
            g = w2[t, pl.ds(n0, TILE), pl.ds(k0, TILE)]
            fold[5 + k, pl.ds(k0, TILE), pl.ds(n0, TILE)] = dot_nt(eye, g).astype(BF16)
        for a in range(0, TILE, LANES):
            for b in range(0, TILE, LANES):
                n_at, k_at = pl.ds(n0 + a, LANES), pl.ds(k0 + b, LANES)

                def add(*taps):
                    terms = [w2[t, n_at, k_at].astype(F32) for t in taps]
                    return terms[0] + terms[1] + terms[2]

                def put(i, v):
                    fold[i, k_at, n_at] = v.astype(BF16).T

                put(3, add(0, 1, 2))
                put(4, add(6, 7, 8))
                left = add(0, 3, 6)
                put(1, left)
                right = add(2, 5, 8)
                put(2, right)
                put(0, left + add(1, 4, 7) + right)
        return carry

    lax.fori_loop(0, tiles * tiles, fold_tile, 0)
    pltpu.make_async_copy(small, small, small_sem).wait()

    def raise_row(i, carry):
        raised[i] = lat[2 + i].astype(F32) + small[2]
        return carry

    lax.fori_loop(0, rows, raise_row, 0)

    same = (
        lax.broadcasted_iota(jnp.int32, (LANES, LANES), 0) // (chans // GROUPS)
        == lax.broadcasted_iota(jnp.int32, (LANES, LANES), 1) // (chans // GROUPS)
    ).astype(F32).astype(BF16)

    pltpu.make_async_copy(stat_in, stat_in, stat_recv).wait()

    total = stat[...] + jnp.sum(stat_in[...], axis=0)
    high = total.astype(BF16).astype(F32)
    rest = total - high
    middle = rest.astype(BF16).astype(F32)
    low = rest - middle
    parts = jnp.concatenate([high, middle, low, jnp.zeros_like(low)], axis=0).astype(BF16)
    sized = dot_nn(parts, same)
    n_stat = 2 * blocks
    total = sized[:n_stat] + sized[n_stat : 2 * n_stat] + sized[2 * n_stat : 3 * n_stat]
    entries = float(own * (chans // GROUPS) * n_view)
    mean = total[:blocks] * (1.0 / entries)
    var = total[blocks:] * (1.0 / entries) - mean * mean
    inv = lax.rsqrt(var + EPSILON)

    def one_row(v):
        return jnp.concatenate([v[k : k + 1] for k in range(blocks)], axis=1)

    scale = one_row(inv) * small[0]
    offset = small[1] - one_row(mean) * scale
    half_scale = scale * 0.5
    half_offset = offset * 0.5

    groups = range(chans // LANES)

    def beside(slot, g, x):
        edge[slot, g, pl.ds(8, cols)] = x
        return edge[slot, g, pl.ds(7, cols)], edge[slot, g, pl.ds(9, cols)]

    def activate(i):
        for g in groups:
            lanes = pl.ds(g * LANES, LANES)
            side = slice(g * LANES, (g + 1) * LANES)
            h = lat[i, :, lanes].astype(F32) * half_scale[:, side] + half_offset[:, side]
            a = h + h * jnp.tanh(h)
            if i < 2:
                a = jnp.where(has_up, a, 0.0)
            if i >= rows + 2:
                a = jnp.where(has_down, a, 0.0)
            left, right = beside(i, g, a)
            act[0, i, :, lanes] = left.astype(BF16)
            act[1, i, :, lanes] = a.astype(BF16)
            act[2, i, :, lanes] = right.astype(BF16)

    pairs = list(range(rows // 2 + 1))
    place = {p: p for p in pairs}

    def arrange(k, pairs):
        a, b = ((0, 2), (1, 2), (2, 1), (1, 3))[k]
        for p in pairs:
            at = pl.ds(place[p] * cols, cols)
            for s in range(3):
                x, y = act[s, 2 * p + a], act[s, 2 * p + b]
                vbuf[k, s, at] = x + y if k == 1 else x - y

    def products(n, k, pairs):
        at = pl.ds(place[pairs[0]] * cols, len(pairs) * cols)
        lanes = pl.ds(n * TILE, TILE)
        terms = [dot_nn(vbuf[k, s, at], gt[k, s, :, lanes]) for s in range(3)]
        mbuf[k, at, lanes] = terms[0] + terms[1] + terms[2]

    bias1 = small[2]

    def mix(n, i):
        p, odd = i // 2, i % 2
        at = pl.ds(place[p] * cols, cols)
        for g in groups[n * TILE // LANES : (n + 1) * TILE // LANES]:
            lanes = pl.ds(g * LANES, LANES)
            v = [mbuf[k, at, lanes] for k in ((1, 2, 3) if odd else (0, 1, 2))]
            conv = v[0] - v[1] - v[2] if odd else v[0] + v[1] + v[2]
            if 1 <= i <= rows:
                m = raised[i - 1, :, lanes] + conv
            else:
                m = lat[i + 1, :, lanes].astype(F32) + conv + bias1[:, g * LANES : (g + 1) * LANES]
            if i == 0:
                m = jnp.where(has_up, m, 0.0)
            if i == rows + 1:
                m = jnp.where(has_down, m, 0.0)
            narrow = m.astype(BF16)
            m = narrow.astype(F32)
            to = pl.ds(i * cols, cols)
            left, right = beside(rows + 4 + i, g, m)
            mx[0, to, lanes] = narrow
            mx[1, to, lanes] = left.astype(BF16) - narrow
            mx[2, to, lanes] = right.astype(BF16) - narrow

    def rise_of(n, j):
        lanes = pl.ds(n * TILE, TILE)
        here, below = pl.ds(j * cols, cols), pl.ds((j + 1) * cols, cols)
        for s in range(3):
            lhs_u[s, here, lanes] = mx[s, below, lanes] - mx[s, here, lanes]

    width = TILE
    bias2 = small[3]

    def take(ref, s, pieces):
        return jnp.concatenate([ref[s, pl.ds(a * cols, b * cols)] for a, b in pieces], axis=0)

    def level(n, pieces):
        lanes = pl.ds(n * width, width)
        mine = [(a + 1, b) for a, b in pieces]
        base = dot_nn(take(mx, 0, mine), fold[0, :, lanes]) + bias2[:, n * width : (n + 1) * width]
        for q in range(2):
            both = base + dot_nn(take(mx, 1 + q, mine), fold[1 + q, :, lanes])
            done = 0
            for a, b in pieces:
                part[n, q, pl.ds(a * cols, b * cols)] = both[done * cols : (done + b) * cols]
                done += b

    def finish(n, p, pieces):
        lanes = pl.ds(n * width, width)
        mine = [(a + p, b) for a, b in pieces]
        rise = dot_nn(take(lhs_u, 0, mine), fold[3 + p, :, lanes])
        for q in range(2):
            term = rise + dot_nn(take(lhs_u, 1 + q, mine), fold[5 + 2 * p + q, :, lanes])
            done = 0
            for a, b in pieces:
                for i in range(a, a + b):
                    for g in range(width // LANES):
                        x = part[n, q, pl.ds(i * cols, cols), pl.ds(g * LANES, LANES)]
                        y = term[done * cols : (done + 1) * cols, g * LANES : (g + 1) * LANES]
                        wide[g, pl.ds((p * rows + i) * 2 * cols + q, cols, 2), :] = x + y if p else x - y
                    done += 1
        for a, b in pieces:
            for i in range(a, a + b):
                for g in range(width // LANES):
                    tile = wide[g, pl.ds((p * rows + i) * 2 * cols, 2 * cols), :].astype(BF16)
                    out_ref[i, p, :, pl.ds(n * width + g * LANES, LANES)] = tile

    columns = range(chans // width)

    own_up.wait()
    own_down.wait()
    for i in range(2, rows + 2, 2):
        activate(i)

    for i in (0, rows + 2):
        activate(i)
    arrange(0, pairs)
    for n in columns:
        products(n, 0, pairs)
    for i in range(1, rows + 4, 2):
        activate(i)
    for n in columns:
        for k in (3, 1, 2):
            if n == 0:
                arrange(k, pairs)
            products(n, k, pairs)
        if n:
            for i in range(rows + 2):
                mix(n - 1, i)
    for i in range(rows + 2):
        mix(columns[-1], i)
    for n in columns:
        for j in range(rows + 1):
            rise_of(n, j)
    for n in columns:
        level(n, [(0, rows)])
        for p in range(2):
            finish(n, p, [(0, rows)])

    pltpu.make_async_copy(stat_in, stat_in, stat_send).wait()

    @pl.when(has_up)
    def _():
        up_copy.wait_send()

    @pl.when(has_down)
    def _():
        down_copy.wait_send()


def per_device(n_view, latents, norm_gain, norm_shift, w_first, bias_first, w_second, bias_second):
    rows, cols, chans = latents.shape
    own = rows * cols
    flat = lambda w: jnp.transpose(w, (1, 2, 0, 3)).reshape(9, chans, chans)
    row = lambda v: v.reshape(1, chans)
    hbm = pl.BlockSpec(memory_space=pl.ANY)
    n_stat = 2 * chans // LANES
    out = pl.pallas_call(
        functools.partial(kernel, n_view, rows, cols, chans),
        out_shape=pltpu.VMEM((rows, 2, 2 * cols, chans), BF16),
        in_specs=[hbm] * 7,
        out_specs=pl.BlockSpec(memory_space=pltpu.VMEM),
        scratch_shapes=[
            pltpu.VMEM((rows + 4, cols, chans), BF16),
            pltpu.VMEM((4, 1, chans), F32),
            pltpu.VMEM((9, chans, chans), BF16),
            pltpu.VMEM((4, 3, chans, chans), BF16),
            pltpu.VMEM((9, chans, chans), BF16),
            pltpu.VMEM((9, chans, chans), BF16),
            pltpu.VMEM((3, rows + 4, cols, chans), BF16),
            pltpu.VMEM((4, 3, (rows // 2 + 1) * cols, chans), BF16),
            pltpu.VMEM((4, (rows // 2 + 1) * cols, chans), F32),
            pltpu.VMEM((3, own + 2 * cols, chans), BF16),
            pltpu.VMEM((3, own + cols, chans), BF16),
            pltpu.VMEM((chans // TILE, 2, own, TILE), F32),
            pltpu.VMEM((TILE // LANES, own * 4, LANES), F32),
            pltpu.VMEM((2 * rows + 6, chans // LANES, cols + 16, LANES), F32),
            pltpu.VMEM((rows, cols, chans), F32),
            pltpu.VMEM((n_stat, LANES), F32),
            pltpu.VMEM((n_view - 1, n_stat, LANES), F32),
            pltpu.SemaphoreType.DMA((rows,)),
            pltpu.SemaphoreType.DMA,
            pltpu.SemaphoreType.DMA((2,)),
            pltpu.SemaphoreType.DMA,
            pltpu.SemaphoreType.DMA((2,)),
            pltpu.SemaphoreType.DMA((2,)),
            pltpu.SemaphoreType.DMA,
            pltpu.SemaphoreType.DMA,
            pltpu.SemaphoreType.REGULAR,
            pltpu.SemaphoreType.REGULAR,
        ],
        compiler_params=pltpu.CompilerParams(
            collective_id=0, has_side_effects=True, vmem_limit_bytes=60 * 1024 * 1024
        ),
    )(
        latents, row(norm_gain), row(norm_shift), flat(w_first), row(bias_first), flat(w_second),
        row(bias_second),
    )
    return out.reshape(2 * rows, 2 * cols, chans)


def solution(mesh):
    placed = (P(("scene", "view"), None, None), P(), P(), P(), P(), P(), P())
    return jax.shard_map(
        functools.partial(per_device, mesh.shape["view"]),
        mesh=mesh,
        in_specs=placed,
        out_specs=P(("scene", "view"), None, None),
        check_vma=False,
    )
```
